8 devices in a mesh: dp: 1 (over z), tp: 2 (over y), cp: 4 (over x, core).
Axes of the slice: x: 2, y: 2, z: 1, core: 2. Of those that a mesh axis runs over, the one named last changes fastest.
Arguments:
- hidden: bfloat16 [4096, 2048], P(('dp', 'cp'))
- positions: int32 [4096], P(('dp', 'cp'))
- ln_gain: bfloat16 [2048], replicated
- w_q: bfloat16 [2048, 2048], P(None, 'tp')
- w_k: bfloat16 [2048, 1024], P(None, 'tp')
- w_v: bfloat16 [2048, 1024], P(None, 'tp')
- w_o: bfloat16 [2048, 2048], P('tp')
- w_gate: bfloat16 [2048, 6144], P(None, 'tp')
- w_up: bfloat16 [2048, 6144], P(None, 'tp')
- w_down: bfloat16 [6144, 2048], P('tp')
Outputs:
- output 1: bfloat16 [4096, 2048], P(('dp', 'cp'))
- output 2: bfloat16 [4096, 8, 128], P(('dp', 'cp'), 'tp')
- output 3: bfloat16 [4096, 8, 128], P(('dp', 'cp'), 'tp')
All inputs are finite; a program needn't handle non-finite values.
Results may differ from the reference program's by a relative error of at most 0.012868.
Values are sent between devices in bfloat16 or wider.
A program may use at most 1 GiB of HBM per device.

```python
import jax
import jax.numpy as jnp
from jax import lax

D_MODEL = 2048
HEADS = 16
KV_HEADS = 8
FF_DIM = 6144
HEAD_DIM = 128
ROPE_BASE = 4000000
TOKENS = 4096
LN_EPS = 1e-5
Q_BLOCK = min(64, TOKENS)


def layer_norm(hidden, ln_gain):
    hidden_f = hidden.astype(jnp.float32)
    row_mean = jnp.mean(hidden_f, axis=-1, keepdims=True)
    centered = hidden_f - row_mean
    row_var = jnp.mean(centered * centered, axis=-1, keepdims=True)
    return (centered * lax.rsqrt(row_var + LN_EPS) * ln_gain.astype(jnp.float32)).astype(jnp.bfloat16)


def rotary(proj, positions):
    half_dim = HEAD_DIM // 2
    inv_freq = 1.0 / (ROPE_BASE ** (jnp.arange(0, HEAD_DIM, 2, dtype=jnp.float32) / HEAD_DIM))
    angles = positions.astype(jnp.float32)[:, None] * inv_freq[None, :]
    bcast_shape = (proj.shape[0],) + (1,) * (proj.ndim - 2) + (half_dim,)
    cosine = jnp.cos(angles).reshape(bcast_shape)
    sine_val = jnp.sin(angles).reshape(bcast_shape)
    paired = proj.astype(jnp.float32).reshape(proj.shape[:-1] + (half_dim, 2))
    even_part = paired[..., 0]
    odd_part = paired[..., 1]
    rotated = jnp.stack([even_part * cosine - odd_part * sine_val, odd_part * cosine + even_part * sine_val], axis=-1)
    return rotated.reshape(proj.shape).astype(jnp.bfloat16)


def setup_inputs(seed: int = 0, part: int = 0) -> dict:
    base_key = jax.random.key(seed)
    part_keys = jax.random.split(jax.random.fold_in(base_key, part), 2)
    weight_keys = jax.random.split(base_key, 8)
    q_width = HEADS * HEAD_DIM
    kv_width = KV_HEADS * HEAD_DIM
    d_scale = D_MODEL ** -0.5
    hidden = jax.random.normal(part_keys[0], (TOKENS, D_MODEL), jnp.float32)
    pos_steps = jax.random.randint(part_keys[1], (TOKENS,), 1, 3, dtype=jnp.int32)
    positions = (jnp.cumsum(pos_steps, dtype=jnp.int32) - pos_steps[0]).astype(jnp.int32)
    ln_gain = 1.0 + 0.3 * jax.random.normal(weight_keys[0], (D_MODEL,), jnp.float32)
    w_q = (1.5 * d_scale) * jax.random.normal(weight_keys[1], (D_MODEL, q_width), jnp.float32)
    w_k = (1.5 * d_scale) * jax.random.normal(weight_keys[2], (D_MODEL, kv_width), jnp.float32)
    w_v = d_scale * jax.random.normal(weight_keys[3], (D_MODEL, kv_width), jnp.float32)
    w_o = (2.0 * q_width ** -0.5) * jax.random.normal(weight_keys[4], (q_width, D_MODEL), jnp.float32)
    w_gate = d_scale * jax.random.normal(weight_keys[5], (D_MODEL, FF_DIM), jnp.float32)
    w_up = d_scale * jax.random.normal(weight_keys[6], (D_MODEL, FF_DIM), jnp.float32)
    w_down = (FF_DIM ** -0.5) * jax.random.normal(weight_keys[7], (FF_DIM, D_MODEL), jnp.float32)
    return {
        'hidden': hidden.astype(jnp.bfloat16),
        'positions': positions,
        'ln_gain': ln_gain.astype(jnp.bfloat16),
        'w_q': w_q.astype(jnp.bfloat16),
        'w_k': w_k.astype(jnp.bfloat16),
        'w_v': w_v.astype(jnp.bfloat16),
        'w_o': w_o.astype(jnp.bfloat16),
        'w_gate': w_gate.astype(jnp.bfloat16),
        'w_up': w_up.astype(jnp.bfloat16),
        'w_down': w_down.astype(jnp.bfloat16),
    }


def reference(hidden, positions, ln_gain, w_q, w_k, w_v, w_o, w_gate, w_up, w_down):
    group_size = HEADS // KV_HEADS
    normed = layer_norm(hidden, ln_gain)
    q_proj = jnp.dot(normed, w_q, preferred_element_type=jnp.float32).astype(jnp.bfloat16)
    k_proj = jnp.dot(normed, w_k, preferred_element_type=jnp.float32).astype(jnp.bfloat16)
    v_cache = jnp.dot(normed, w_v, preferred_element_type=jnp.float32).astype(jnp.bfloat16).reshape(TOKENS, KV_HEADS, HEAD_DIM)
    q_rot = rotary(q_proj.reshape(TOKENS, KV_HEADS, group_size, HEAD_DIM), positions)
    k_cache = rotary(k_proj.reshape(TOKENS, KV_HEADS, HEAD_DIM), positions)
    k_float = k_cache.astype(jnp.float32)
    v_float = v_cache.astype(jnp.float32)
    key_pos = jnp.arange(TOKENS)
    score_scale = HEAD_DIM ** -0.5
    q_blocks = q_rot.reshape(TOKENS // Q_BLOCK, Q_BLOCK, KV_HEADS, group_size, HEAD_DIM)

    def attend_block(block_args):
        block_id, q_block = block_args
        scores = jnp.einsum('qkgd,tkd->qkgt', q_block.astype(jnp.float32), k_float) * score_scale
        query_pos = block_id * Q_BLOCK + jnp.arange(Q_BLOCK)
        allowed = key_pos[None, :] <= query_pos[:, None]
        scores = jnp.where(allowed[:, None, None, :], scores, -jnp.inf)
        row_max = jnp.max(scores, axis=-1, keepdims=True)
        weights = jnp.exp(scores - row_max)
        row_sum = jnp.sum(weights, axis=-1, keepdims=True)
        probs = weights.astype(jnp.bfloat16).astype(jnp.float32)
        numer = jnp.einsum('qkgt,tkd->qkgd', probs, v_float)
        return (numer / row_sum).astype(jnp.bfloat16)

    attn = lax.map(attend_block, (jnp.arange(TOKENS // Q_BLOCK), q_blocks))
    attn_flat = attn.reshape(TOKENS, HEADS * HEAD_DIM)
    attn_out = jnp.dot(attn_flat, w_o, preferred_element_type=jnp.float32)
    gate_proj = jnp.dot(normed, w_gate, preferred_element_type=jnp.float32).astype(jnp.bfloat16)
    up_proj = jnp.dot(normed, w_up, preferred_element_type=jnp.float32).astype(jnp.bfloat16)
    mlp_act = (jax.nn.silu(gate_proj.astype(jnp.float32)) * up_proj.astype(jnp.float32)).astype(jnp.bfloat16)
    mlp_out = jnp.dot(mlp_act, w_down, preferred_element_type=jnp.float32)
    hidden_out = (hidden.astype(jnp.float32) + attn_out + mlp_out).astype(jnp.bfloat16)
    return (hidden_out, k_cache, v_cache)
```

```python
import functools
import math

import jax
import jax.numpy as jnp
from jax import lax
from jax.experimental import pallas as pl
from jax.experimental.pallas import tpu as pltpu
from jax.sharding import PartitionSpec as P


HEAD_DIM = 128
ROPE_BASE = 4000000
LN_EPS = 1e-5
F32 = jnp.float32
BF16 = jnp.bfloat16
VMEM_LIMIT = 67043328
CHUNKS = (128, 256, 256, 256, 128)


def params(*semantics):
    return pltpu.CompilerParams(dimension_semantics=semantics, vmem_limit_bytes=VMEM_LIMIT)


def cost(flops, nbytes):
    return pl.CostEstimate(flops=int(flops), bytes_accessed=int(nbytes), transcendentals=0)


def norm_v_kernel(x_ref, g_ref, wv_ref, h_ref, v_ref, vt_ref):
    x = x_ref[...].astype(F32)
    mean = jnp.mean(x, axis=-1, keepdims=True)
    cent = x - mean
    var = jnp.mean(cent * cent, axis=-1, keepdims=True)
    h = (cent * lax.rsqrt(var + LN_EPS) * g_ref[...].astype(F32)).astype(BF16)
    h_ref[...] = h
    v = jnp.dot(h, wv_ref[...], preferred_element_type=F32).astype(BF16)
    v_ref[...] = v
    vt_ref[...] = v.T


def norm_v(hidden, gain, w_v):
    rows, width = hidden.shape
    cols = w_v.shape[1]
    blk = 256
    return pl.pallas_call(
        norm_v_kernel,
        grid=(rows // blk,),
        in_specs=[
            pl.BlockSpec((blk, width), lambda i: (i, 0)),
            pl.BlockSpec((1, width), lambda i: (0, 0)),
            pl.BlockSpec((width, cols), lambda i: (0, 0)),
        ],
        out_specs=[
            pl.BlockSpec((blk, width), lambda i: (i, 0)),
            pl.BlockSpec((blk, cols), lambda i: (i, 0)),
            pl.BlockSpec((cols, blk), lambda i: (0, i)),
        ],
        out_shape=[
            jax.ShapeDtypeStruct((rows, width), BF16),
            jax.ShapeDtypeStruct((rows, cols), BF16),
            jax.ShapeDtypeStruct((cols, rows), BF16),
        ],
        compiler_params=params("arbitrary"),
        cost_estimate=cost(2 * rows * width * cols, 4 * rows * width + 2 * width * cols),
        name="norm_v",
    )(hidden, gain.reshape(1, width), w_v)


def rope_proj_kernel(h_ref, w_ref, cos_ref, sin_ref, swap_ref, out_ref):
    proj = jnp.dot(h_ref[...], w_ref[...], preferred_element_type=F32).astype(BF16)
    swapped = jnp.dot(proj, swap_ref[...], preferred_element_type=F32)
    cos = cos_ref[...]
    sin = sin_ref[...]
    for j in range(proj.shape[1] // HEAD_DIM):
        cols = slice(j * HEAD_DIM, (j + 1) * HEAD_DIM)
        out_ref[:, cols] = (proj[:, cols].astype(F32) * cos + swapped[:, cols] * sin).astype(BF16)


def rope_proj(h, w, cos, sin, swap):
    rows, width = h.shape
    cols = w.shape[1]
    blk = 256
    return pl.pallas_call(
        rope_proj_kernel,
        grid=(cols // blk,),
        in_specs=[
            pl.BlockSpec((rows, width), lambda i: (0, 0)),
            pl.BlockSpec((width, blk), lambda i: (0, i)),
            pl.BlockSpec((rows, HEAD_DIM), lambda i: (0, 0)),
            pl.BlockSpec((rows, HEAD_DIM), lambda i: (0, 0)),
            pl.BlockSpec((blk, blk), lambda i: (0, 0)),
        ],
        out_specs=pl.BlockSpec((rows, blk), lambda i: (0, i)),
        out_shape=jax.ShapeDtypeStruct((rows, cols), BF16),
        compiler_params=params("arbitrary"),
        cost_estimate=cost(2 * rows * width * cols, 2 * rows * (width + cols) + 2 * width * cols),
    )(h, w, cos, sin, swap)


def gate_up_kernel(h_ref, wg_ref, wu_ref, *refs):
    h = h_ref[...]
    gate = jnp.dot(h, wg_ref[...], preferred_element_type=F32).astype(BF16).astype(F32)
    up = jnp.dot(h, wu_ref[...], preferred_element_type=F32).astype(BF16).astype(F32)
    refs[-1][...] = (jax.nn.silu(gate) * up).astype(BF16)


def gate_up(h, w_gate, w_up, first, last, out):
    rows, width = h.shape
    cols = w_gate.shape[1]
    blk = 256
    specs = [
        pl.BlockSpec((rows, width), lambda i: (0, 0)),
        pl.BlockSpec((width, blk), lambda i: (0, first + i)),
        pl.BlockSpec((width, blk), lambda i: (0, first + i)),
    ]
    operands = [h, w_gate, w_up]
    aliases = {}
    if out is not None:
        specs.append(pl.BlockSpec(memory_space=pl.ANY))
        operands.append(out)
        aliases = {3: 0}
    done = (last - first) * blk
    return pl.pallas_call(
        gate_up_kernel,
        grid=(last - first,),
        in_specs=specs,
        out_specs=pl.BlockSpec((rows, blk), lambda i: (0, first + i)),
        out_shape=jax.ShapeDtypeStruct((rows, cols), BF16),
        input_output_aliases=aliases,
        compiler_params=params("arbitrary"),
        cost_estimate=cost(4 * rows * width * done, 2 * rows * (width + done) + 4 * width * done),
        name="gate_up",
    )(*operands)


def chunk_kernel(row0, rows, q_ref, k0, v0, k1, v1, k2, v2, k3, v3, a_ref, wo_ref, wd_ref,
                 out_ref, max_ref, sum_ref, acc_ref, part_ref):
    step = pl.program_id(0)
    me = lax.axis_index("cp")
    scale = HEAD_DIM ** -0.5 * math.log2(math.e)
    q = jnp.concatenate([q_ref[:, :HEAD_DIM], q_ref[:, HEAD_DIM:]], axis=0)

    def scores(k):
        return lax.dot_general(k, q, (((1,), (1,)), ((), ())), preferred_element_type=F32) * scale

    diag = scores(k0[row0:row0 + rows, :])
    key_id = lax.broadcasted_iota(jnp.int32, diag.shape, 0)
    query_id = lax.broadcasted_iota(jnp.int32, diag.shape, 1) % rows
    diag = jnp.where(key_id <= query_id, diag, -jnp.inf)
    top = jnp.max(diag, axis=0, keepdims=True)
    if row0:
        rest = scores(k0[:row0, :])
        top = jnp.maximum(top, jnp.max(rest, axis=0, keepdims=True))
    weight = jnp.exp2(diag - top)
    total = jnp.sum(weight, axis=0, keepdims=True)
    acc = jnp.dot(v0[:, row0:row0 + rows], weight.astype(BF16), preferred_element_type=F32)
    if row0:
        weight = jnp.exp2(rest - top)
        total += jnp.sum(weight, axis=0, keepdims=True)
        acc += jnp.dot(v0[:, :row0], weight.astype(BF16), preferred_element_type=F32)
    max_ref[...] = top
    sum_ref[...] = total
    acc_ref[...] = acc

    def other(k_ref, v_ref):
        s = scores(k_ref[...])
        old = max_ref[...]
        new = jnp.maximum(old, jnp.max(s, axis=0, keepdims=True))
        factor = jnp.exp2(old - new)
        weight = jnp.exp2(s - new)
        sum_ref[...] = sum_ref[...] * factor + jnp.sum(weight, axis=0, keepdims=True)
        acc_ref[...] = acc_ref[...] * factor + jnp.dot(v_ref[...], weight.astype(BF16), preferred_element_type=F32)
        max_ref[...] = new

    @pl.when(me % 2 == 1)
    def _():
        other(k1, v1)

    @pl.when(me >= 2)
    def _():
        other(k2, v2)
        other(k3, v3)

    o = (acc_ref[...] / sum_ref[...]).T.astype(BF16)
    o = jnp.concatenate([o[:rows, :], o[rows:, :]], axis=1)
    part = jnp.dot(o, wo_ref[...], preferred_element_type=F32)
    part += jnp.dot(a_ref[...], wd_ref[...], preferred_element_type=F32)

    @pl.when(step == 0)
    def _():
        part_ref[...] = part

    @pl.when(step > 0)
    def _():
        part_ref[...] += part

    @pl.when(step == pl.num_programs(0) - 1)
    def _():
        out_ref[...] = part_ref[...].astype(BF16)


def chunk_part(row0, rows, q, sources, act, w_o, w_down):
    tok_rows = q.shape[0]
    kv_heads = q.shape[1] // (2 * HEAD_DIM)
    width = w_o.shape[1]
    ff_blk = act.shape[1] // kv_heads
    q = q[row0:row0 + rows]
    act = act[row0:row0 + rows]
    kv_specs = []
    operands = []
    for k, vt in sources:
        kv_specs += [pl.BlockSpec((tok_rows, HEAD_DIM), lambda g: (0, g)), pl.BlockSpec((HEAD_DIM, tok_rows), lambda g: (g, 0))]
        operands += [k, vt]
    return pl.pallas_call(
        functools.partial(chunk_kernel, row0, rows),
        grid=(kv_heads,),
        in_specs=[pl.BlockSpec((rows, 2 * HEAD_DIM), lambda g: (0, g))] + kv_specs + [
            pl.BlockSpec((rows, ff_blk), lambda g: (0, g)),
            pl.BlockSpec((2 * HEAD_DIM, width), lambda g: (g, 0)),
            pl.BlockSpec((ff_blk, width), lambda g: (g, 0)),
        ],
        out_specs=pl.BlockSpec((rows, width), lambda g: (0, 0)),
        out_shape=jax.ShapeDtypeStruct((rows, width), BF16),
        scratch_shapes=[
            pltpu.VMEM((1, 2 * rows), F32),
            pltpu.VMEM((1, 2 * rows), F32),
            pltpu.VMEM((HEAD_DIM, 2 * rows), F32),
            pltpu.VMEM((rows, width), F32),
        ],
        compiler_params=params("arbitrary"),
        cost_estimate=cost(2 * rows * (width * (act.shape[1] + q.shape[1]) + 8 * tok_rows * q.shape[1]), 30e6),
        name="chunk_part",
    )(q, *operands, act, w_o, w_down)


def add_kernel(x_ref, p_ref, r_ref, *refs):
    refs[-1][...] = (x_ref[...].astype(F32) + (p_ref[...].astype(F32) + r_ref[...].astype(F32))).astype(BF16)


def add_chunk(row0, hidden, part, recv, out):
    rows, width = part.shape
    blk = 128
    first = row0 // blk
    specs = [
        pl.BlockSpec((blk, width), lambda i: (first + i, 0)),
        pl.BlockSpec((blk, width), lambda i: (i, 0)),
        pl.BlockSpec((blk, width), lambda i: (i, 0)),
    ]
    operands = [hidden, part, recv]
    aliases = {}
    if out is not None:
        specs.append(pl.BlockSpec(memory_space=pl.ANY))
        operands.append(out)
        aliases = {3: 0}
    return pl.pallas_call(
        add_kernel,
        grid=(rows // blk,),
        in_specs=specs,
        out_specs=pl.BlockSpec((blk, width), lambda i: (first + i, 0)),
        out_shape=jax.ShapeDtypeStruct(hidden.shape, BF16),
        input_output_aliases=aliases,
        compiler_params=params("arbitrary"),
        cost_estimate=cost(4 * rows * width, 8 * rows * width),
        name="add_chunk",
    )(*operands)


def rope_tables(positions):
    lane = jnp.arange(HEAD_DIM)
    exponent = (lane - lane % 2).astype(F32) / HEAD_DIM
    inv_freq = 1.0 / (ROPE_BASE ** exponent)
    angles = positions.astype(F32)[:, None] * inv_freq[None, :]
    sign = jnp.where(lane % 2 == 0, -1.0, 1.0).astype(F32)
    return jnp.cos(angles), jnp.sin(angles) * sign[None, :]


def solution(mesh):
    def layer(hidden, positions, ln_gain, w_q, w_k, w_v, w_o, w_gate, w_up, w_down):
        tok_rows = hidden.shape[0]
        kv_local = w_k.shape[1] // HEAD_DIM
        cross = lambda t: lax.ppermute(t, 'cp', [(0, 2), (1, 3)])
        upward = lambda t: lax.ppermute(t, 'cp', [(0, 1), (2, 3)])
        relay = lambda t: lax.ppermute(t, 'cp', [(2, 3), (3, 2)])

        h, v, vt = norm_v(hidden, ln_gain, w_v)
        vt_x = cross(vt)
        positions, h = lax.optimization_barrier((positions, h))
        cos, sin = rope_tables(positions)
        row = jnp.arange(2 * HEAD_DIM)
        swap = (row[:, None] == (row ^ 1)[None, :]).astype(BF16)
        k = rope_proj(h, w_k, cos, sin, swap)
        k_x = cross(k)
        h, k = lax.optimization_barrier((h, k))
        vt_u = upward(vt)
        k_u = upward(k)
        q = rope_proj(h, w_q, cos, sin, swap)
        h, q = lax.optimization_barrier((h, q))
        act = gate_up(h, w_gate, w_up, 0, 6, None)
        vt_r = relay(vt_x)
        act = gate_up(h, w_gate, w_up, 6, 12, act)
        k_r = relay(k_x)
        sources = ((k, vt), (k_u, vt_u), (k_x, vt_x), (k_r, vt_r))
        parts = []
        row0 = 0
        for rows in CHUNKS:
            part = chunk_part(row0, rows, q, sources, act, w_o, w_down)
            recv = lax.ppermute(part, 'tp', [(0, 1), (1, 0)])
            q, part, act = lax.optimization_barrier((q, part, act))
            parts.append((row0, part, recv))
            row0 += rows
        out = None
        for row0, part, recv in parts:
            out = add_chunk(row0, hidden, part, recv, out)
        shape = (tok_rows, kv_local, HEAD_DIM)
        return out, k.reshape(shape), v.reshape(shape)

    row_spec = P(('dp', 'cp'), None)
    col_spec = P(None, 'tp')
    cache_spec = P(('dp', 'cp'), 'tp', None)
    in_specs = (row_spec, P(('dp', 'cp')), P(None), col_spec, col_spec, col_spec, P('tp', None), col_spec, col_spec, P('tp', None))
    return jax.shard_map(layer, mesh=mesh, in_specs=in_specs, out_specs=(row_spec, cache_spec, cache_spec), check_vma=False)
```

```python
import functools
import math

import jax
import jax.numpy as jnp
from jax import lax
from jax.experimental import pallas as pl
from jax.experimental.pallas import tpu as pltpu
from jax.sharding import PartitionSpec as P

HEAD_DIM = 128
ROPE_BASE = 4000000
LN_EPS = 1e-5
F32 = jnp.float32
BF16 = jnp.bfloat16
MESH = pl.DeviceIdType.MESH
VMEM_LIMIT = 67043328

WBLK = 256
RING = 8
RBLK = 256
CHUNK = 128
KEYS = 512


def layer_kernel(x_hbm, gain_ref, cos_ref, sin_ref, wq_hbm, wk_hbm, wv_hbm, wo_hbm, wg_hbm, wu_hbm, wd_hbm,
                 out_hbm, k_hbm, v_hbm,
                 x_buf, h_buf, ring, act, q_buf, k_all, vt_all, v_own, wo, wd, recv, mlp, qs, o_buf, top_ref, sum_ref, acc_ref,
                 x_sem, ring_sem, wo_sem, wd_sem, kv_sem, out_sem,
                 cross_send, cross_recv, up_send, up_recv, relay_send, relay_recv, part_send, part_recv):
    me = lax.axis_index("cp")
    tp = lax.axis_index("tp")
    odd = me % 2
    partner = me + 1 - 2 * odd
    across = (me + 2) % 4
    rows, width = x_buf.shape
    kv_heads = k_all.shape[1] // HEAD_DIM
    n_rblk = rows // RBLK
    n_chunk = rows // CHUNK
    n_ff = act.shape[1] // WBLK
    part = h_buf

    def x_copy(b):
        r = pl.ds(pl.multiple_of(b * RBLK, RBLK), RBLK)
        return pltpu.make_async_copy(x_hbm.at[r, :], x_buf.at[r, :], x_sem.at[b])

    def w_copy(w_hbm, blk, slot):
        c = pl.ds(pl.multiple_of(blk * WBLK, WBLK), WBLK)
        return pltpu.make_async_copy(w_hbm.at[:, c], ring.at[slot], ring_sem.at[slot])

    wo_copy = pltpu.make_async_copy(wo_hbm, wo, wo_sem)
    wd_copy = pltpu.make_async_copy(wd_hbm, wd, wd_sem)

    x_copy(0).start()
    w_copy(wv_hbm, 0, 0).start()
    w_copy(wv_hbm, 1, 1).start()
    for b in range(1, n_rblk):
        x_copy(b).start()
    w_copy(wk_hbm, 0, 2).start()
    w_copy(wk_hbm, 1, 3).start()
    for j in range(4):
        w_copy(wq_hbm, j, 4 + j).start()

    barrier = pltpu.get_barrier_semaphore()
    pl.semaphore_signal(barrier, inc=1, device_id={"tp": 1 - tp}, device_id_type=MESH)
    pl.semaphore_signal(barrier, inc=1, device_id={"cp": partner}, device_id_type=MESH)
    pl.semaphore_signal(barrier, inc=1, device_id={"cp": across}, device_id_type=MESH)

    def region(owner, kind, b):
        at = pl.ds(pl.multiple_of(owner * rows + b * RBLK, RBLK), RBLK)
        return k_all.at[at, :] if kind else vt_all.at[:, at]

    def kv_copy(owner, kind, b, sends, recvs, target):
        ref = region(owner, kind, b)
        i = kind * n_rblk + b
        return pltpu.make_async_remote_copy(ref, ref, sends.at[i], recvs.at[i], device_id={"cp": target}, device_id_type=MESH)

    def cross(owner, kind, b):
        return kv_copy(owner, kind, b, cross_send, cross_recv, (owner + 2) % 4)

    def up(owner, kind, b):
        return kv_copy(owner, kind, b, up_send, up_recv, (owner + 1) % 4)

    def relay(owner, kind, b):
        return kv_copy(owner, kind, b, relay_send, relay_recv, 3 - owner)

    def send_piece(kind, b):
        @pl.when(me < 2)
        def _():
            cross(me, kind, b).start()

        @pl.when(odd == 0)
        def _():
            up(me, kind, b).start()

    def relay_piece(kind, b):
        owner = me - 2
        cross(owner, kind, b).wait_recv()
        kv_copy(owner, kind, b, relay_send, relay_recv, partner).start()

    def part_copy(c):
        r = pl.ds(pl.multiple_of(c * CHUNK, CHUNK), CHUNK)
        return pltpu.make_async_remote_copy(part.at[r, :], recv.at[r, :], part_send.at[c], part_recv.at[c],
                                            device_id={"tp": 1 - tp}, device_id_type=MESH)

    w_copy(wv_hbm, 0, 0).wait()
    w_copy(wv_hbm, 1, 1).wait()

    @pl.loop(0, n_rblk)
    def _(b):
        x_copy(b).wait()
        r = pl.ds(pl.multiple_of(b * RBLK, RBLK), RBLK)
        x = x_buf[r, :].astype(F32)
        mean = jnp.mean(x, axis=-1, keepdims=True)
        cent = x - mean
        var = jnp.mean(cent * cent, axis=-1, keepdims=True)
        h = (cent * lax.rsqrt(var + LN_EPS) * gain_ref[...].astype(F32)).astype(BF16)
        h_buf[r, :] = h
        for j in range(2):
            v = jnp.dot(h, ring[j], preferred_element_type=F32).astype(BF16)
            v_own[r, j * WBLK:(j + 1) * WBLK] = v
            at = pl.ds(pl.multiple_of(me * rows + b * RBLK, RBLK), RBLK)
            vt_all[j * WBLK:(j + 1) * WBLK, at] = v.T

        @pl.when(b == 0)
        def _():
            pl.semaphore_wait(barrier, 3)

        send_piece(0, b)

    v_out = pltpu.make_async_copy(v_own, v_hbm, kv_sem.at[0])
    v_out.start()

    lane = lax.broadcasted_iota(jnp.int32, (WBLK, WBLK), 0)
    other = lax.broadcasted_iota(jnp.int32, (WBLK, WBLK), 1)
    swap = jnp.where(lane == other + 1 - 2 * (other % 2), 1.0, 0.0).astype(BF16)

    def rope(r, w):
        proj = jnp.dot(h_buf[r, :], w, preferred_element_type=F32).astype(BF16)
        swapped = jnp.dot(proj, swap, preferred_element_type=F32)
        cos = cos_ref[r, :]
        sin = sin_ref[r, :]
        halves = []
        for i in range(WBLK // HEAD_DIM):
            c = slice(i * HEAD_DIM, (i + 1) * HEAD_DIM)
            halves.append((proj[:, c].astype(F32) * cos + swapped[:, c] * sin).astype(BF16))
        return jnp.concatenate(halves, axis=1)

    w_copy(wk_hbm, 0, 2).wait()
    w_copy(wk_hbm, 1, 3).wait()

    @pl.loop(0, n_rblk)
    def _(b):
        r = pl.ds(pl.multiple_of(b * RBLK, RBLK), RBLK)
        at = pl.ds(pl.multiple_of(me * rows + b * RBLK, RBLK), RBLK)
        for j in range(2):
            k_all[at, j * WBLK:(j + 1) * WBLK] = rope(r, ring[2 + j])
        send_piece(1, b)

    k_out = pltpu.make_async_copy(k_all.at[pl.ds(pl.multiple_of(me * rows, RBLK), rows), :], k_hbm, kv_sem.at[1])
    k_out.start()

    def ff_copies(s):
        slot = 2 * (s % 4)
        return w_copy(wg_hbm, s, slot), w_copy(wu_hbm, s, slot + 1)

    for s in range(2):
        for copy in ff_copies(s):
            copy.start()

    @pl.loop(0, 4)
    def _(j):
        w_copy(wq_hbm, j, 4 + j).wait()
        for b in range(n_rblk):
            r = slice(b * RBLK, (b + 1) * RBLK)
            q_buf[r, pl.ds(pl.multiple_of(j * WBLK, WBLK), WBLK)] = rope(r, ring[4 + j])

    for s in range(2, 4):
        for copy in ff_copies(s):
            copy.start()
    wo_copy.start()
    wd_copy.start()

    @pl.loop(0, n_ff)
    def _(s):
        for copy in ff_copies(s):
            copy.wait()
        slot = 2 * (s % 4)
        for b in range(n_rblk):
            r = slice(b * RBLK, (b + 1) * RBLK)
            h = h_buf[r, :]
            gate = jnp.dot(h, ring[slot], preferred_element_type=F32).astype(BF16).astype(F32)
            up_ = jnp.dot(h, ring[slot + 1], preferred_element_type=F32).astype(BF16).astype(F32)
            act[r, pl.ds(pl.multiple_of(s * WBLK, WBLK), WBLK)] = (jax.nn.silu(gate) * up_).astype(BF16)

        @pl.when(s + 4 < n_ff)
        def _():
            for copy in ff_copies(s + 4):
                copy.start()

        @pl.when((me >= 2) & (s >= 2) & (s < 6))
        def _():
            relay_piece(0, s - 2)

        @pl.when((me >= 2) & (s >= 7) & (s % 2 == 1))
        def _():
            relay_piece(1, (s - 7) // 2)

    def down(c):
        r = pl.ds(pl.multiple_of(c * CHUNK, CHUNK), CHUNK)
        a = act[r, :]
        for j in range(4):
            cols = slice(j * (width // 4), (j + 1) * (width // 4))
            mlp[:, cols] = jnp.dot(a, wd[:, cols], preferred_element_type=F32)

    wo_copy.wait()
    wd_copy.wait()
    down(0)

    @pl.when(me >= 2)
    def _():
        relay_piece(1, 3)
        for kind in range(2):
            for b in range(n_rblk):
                kv_copy(3 - me, kind, b, relay_send, relay_recv, partner).wait_recv()

    @pl.when(odd == 1)
    def _():
        for kind in range(2):
            for b in range(n_rblk):
                up(me - 1, kind, b).wait_recv()

    scale = HEAD_DIM ** -0.5 * math.log2(math.e)

    def attend(j, first):
        at = pl.ds(pl.multiple_of(j * KEYS, KEYS), KEYS)
        for g in range(kv_heads):
            heads = slice(g * HEAD_DIM, (g + 1) * HEAD_DIM)
            s = lax.dot_general(k_all[at, heads], qs[g], (((1,), (1,)), ((), ())), preferred_element_type=F32) * scale
            if first is not None:
                key_id = lax.broadcasted_iota(jnp.int32, s.shape, 0)
                query_id = lax.broadcasted_iota(jnp.int32, s.shape, 1) % CHUNK
                s = jnp.where(key_id <= query_id + first, s, -jnp.inf)
            old = top_ref[g]
            new = jnp.maximum(old, jnp.max(s, axis=0, keepdims=True))
            factor = jnp.exp2(old - new)
            weight = jnp.exp2(s - new)
            top_ref[g] = new
            sum_ref[g] = sum_ref[g] * factor + jnp.sum(weight, axis=0, keepdims=True)
            acc_ref[g] = acc_ref[g] * factor + jnp.dot(vt_all[heads, at], weight.astype(BF16), preferred_element_type=F32)

    @pl.loop(0, n_chunk)
    def _(c):
        r = pl.ds(pl.multiple_of(c * CHUNK, CHUNK), CHUNK)
        for g in range(kv_heads):
            for i in range(2):
                col = (2 * g + i) * HEAD_DIM
                qs[g, i * CHUNK:(i + 1) * CHUNK, :] = q_buf[r, col:col + HEAD_DIM]
        top_ref[...] = jnp.full_like(top_ref, -jnp.inf)
        sum_ref[...] = jnp.zeros_like(sum_ref)
        acc_ref[...] = jnp.zeros_like(acc_ref)
        full = me * (rows // KEYS) + c // (KEYS // CHUNK)

        @pl.loop(0, full)
        def _(j):
            attend(j, None)

        attend(full, (c % (KEYS // CHUNK)) * CHUNK)
        for g in range(kv_heads):
            o = (acc_ref[g] / sum_ref[g]).T.astype(BF16)
            for i in range(2):
                col = (2 * g + i) * HEAD_DIM
                o_buf[:, col:col + HEAD_DIM] = o[i * CHUNK:(i + 1) * CHUNK, :]
        o = o_buf[...]
        for j in range(4):
            cols = slice(j * (width // 4), (j + 1) * (width // 4))
            part[r, cols] = (jnp.dot(o, wo[:, cols], preferred_element_type=F32) + mlp[:, cols]).astype(BF16)
        part_copy(c).start()

        @pl.when(c + 1 < n_chunk)
        def _():
            down(c + 1)

    def out_copy(c):
        r = pl.ds(pl.multiple_of(c * CHUNK, CHUNK), CHUNK)
        return pltpu.make_async_copy(x_buf.at[r, :], out_hbm.at[r, :], out_sem.at[c])

    @pl.loop(0, n_chunk)
    def _(c):
        r = pl.ds(pl.multiple_of(c * CHUNK, CHUNK), CHUNK)
        part_copy(c).wait_recv()
        x_buf[r, :] = (x_buf[r, :].astype(F32) + (part[r, :].astype(F32) + recv[r, :].astype(F32))).astype(BF16)
        out_copy(c).start()

    @pl.loop(0, n_chunk)
    def _(c):
        out_copy(c).wait()
        part_copy(c).wait_send()

    v_out.wait()
    k_out.wait()
    for kind in range(2):
        for b in range(n_rblk):
            @pl.when(me < 2)
            def _():
                cross(me, kind, b).wait_send()

            @pl.when(odd == 0)
            def _():
                up(me, kind, b).wait_send()

            @pl.when(me >= 2)
            def _():
                kv_copy(me - 2, kind, b, relay_send, relay_recv, partner).wait_send()


def rope_tables(positions):
    lane = jnp.arange(HEAD_DIM)
    exponent = (lane - lane % 2).astype(F32) / HEAD_DIM
    inv_freq = 1.0 / (ROPE_BASE ** exponent)
    angles = positions.astype(F32)[:, None] * inv_freq[None, :]
    sign = jnp.where(lane % 2 == 0, -1.0, 1.0).astype(F32)
    return jnp.cos(angles), jnp.sin(angles) * sign[None, :]


def solution(mesh):
    n_cp = mesh.shape['cp']

    def local_layer(hidden, positions, ln_gain, w_q, w_k, w_v, w_o, w_gate, w_up, w_down):
        rows, width = hidden.shape
        q_cols = w_q.shape[1]
        kv_cols = w_k.shape[1]
        ff = w_gate.shape[1]
        kv_heads = kv_cols // HEAD_DIM
        keys = n_cp * rows
        n_chunk = rows // CHUNK
        pieces = 2 * (rows // RBLK)
        cos, sin = rope_tables(positions)
        hbm = pl.BlockSpec(memory_space=pl.ANY)
        vmem = pl.BlockSpec(memory_space=pltpu.VMEM)
        dma = pltpu.SemaphoreType.DMA
        out, k, v = pl.pallas_call(
            layer_kernel,
            in_specs=[hbm, vmem, vmem, vmem] + [hbm] * 7,
            out_specs=[hbm] * 3,
            out_shape=[
                jax.ShapeDtypeStruct((rows, width), BF16),
                jax.ShapeDtypeStruct((rows, kv_cols), BF16),
                jax.ShapeDtypeStruct((rows, kv_cols), BF16),
            ],
            scratch_shapes=[
                pltpu.VMEM((rows, width), BF16),
                pltpu.VMEM((rows, width), BF16),
                pltpu.VMEM((RING, width, WBLK), BF16),
                pltpu.VMEM((rows, ff), BF16),
                pltpu.VMEM((rows, q_cols), BF16),
                pltpu.VMEM((keys, kv_cols), BF16),
                pltpu.VMEM((kv_cols, keys), BF16),
                pltpu.VMEM((rows, kv_cols), BF16),
                pltpu.VMEM((q_cols, width), BF16),
                pltpu.VMEM((ff, width), BF16),
                pltpu.VMEM((rows, width), BF16),
                pltpu.VMEM((CHUNK, width), F32),
                pltpu.VMEM((kv_heads, 2 * CHUNK, HEAD_DIM), BF16),
                pltpu.VMEM((CHUNK, q_cols), BF16),
                pltpu.VMEM((kv_heads, 1, 2 * CHUNK), F32),
                pltpu.VMEM((kv_heads, 1, 2 * CHUNK), F32),
                pltpu.VMEM((kv_heads, HEAD_DIM, 2 * CHUNK), F32),
                dma((rows // RBLK,)), dma((RING,)), dma, dma, dma((2,)), dma((n_chunk,)),
                dma((pieces,)), dma((pieces,)), dma((pieces,)), dma((pieces,)), dma((pieces,)), dma((pieces,)),
                dma((n_chunk,)), dma((n_chunk,)),
            ],
            compiler_params=pltpu.CompilerParams(collective_id=0, has_side_effects=True, vmem_limit_bytes=VMEM_LIMIT),
            name="layer",
        )(hidden, ln_gain.reshape(1, width), cos, sin, w_q, w_k, w_v, w_o, w_gate, w_up, w_down)
        shape = (rows, kv_heads, HEAD_DIM)
        return out, k.reshape(shape), v.reshape(shape)

    row_spec = P(('dp', 'cp'), None)
    col_spec = P(None, 'tp')
    cache_spec = P(('dp', 'cp'), 'tp', None)
    in_specs = (row_spec, P(('dp', 'cp')), P(None), col_spec, col_spec, col_spec, P('tp', None), col_spec, col_spec, P('tp', None))
    return jax.shard_map(local_layer, mesh=mesh, in_specs=in_specs, out_specs=(row_spec, cache_spec, cache_spec), check_vma=False)
```

```python
import functools
import math

import jax
import jax.numpy as jnp
from jax import lax
from jax.experimental import pallas as pl
from jax.experimental.pallas import tpu as pltpu
from jax.sharding import PartitionSpec as P

HEAD_DIM = 128
ROPE_BASE = 4000000
LN_EPS = 1e-5
F32 = jnp.float32
BF16 = jnp.bfloat16
MESH = pl.DeviceIdType.MESH
VMEM_LIMIT = 67043328

WBLK = 256
RING = 8
RBLK = 256
CHUNK = 128
KEYS = 512
VIA = 1
VIA_AFTER = 5
VIA_PIECES = 4


def layer_kernel(x_hbm, gain_ref, cos_ref, sin_ref, wq_hbm, wk_hbm, wv_hbm, wo_hbm, wg_hbm, wu_hbm, wd_hbm,
                 out_hbm, k_hbm, v_hbm,
                 x_buf, h_buf, ring, act, q_buf, k_all, vt_all, v_own, wo, wd, recv, mlp, qs, o_buf, s_ref, blk_ref, top_ref, sum_ref, acc_ref,
                 x_sem, ring_sem, wo_sem, wd_sem, kv_sem, out_sem,
                 cross_send, cross_recv, up_send, up_recv, relay_send, relay_recv, part_send, part_recv, via, via_send, via_recv):
    me = lax.axis_index("cp")
    tp = lax.axis_index("tp")
    odd = me % 2
    partner = me + 1 - 2 * odd
    across = (me + 2) % 4
    rows, width = x_buf.shape
    kv_heads = k_all.shape[1] // HEAD_DIM
    n_rblk = rows // RBLK
    n_chunk = rows // CHUNK
    n_ff = act.shape[1] // WBLK
    part = h_buf

    def x_copy(b):
        r = pl.ds(pl.multiple_of(b * RBLK, RBLK), RBLK)
        return pltpu.make_async_copy(x_hbm.at[r, :], x_buf.at[r, :], x_sem.at[b])

    def w_copy(w_hbm, blk, slot):
        c = pl.ds(pl.multiple_of(blk * WBLK, WBLK), WBLK)
        return pltpu.make_async_copy(w_hbm.at[:, c], ring.at[slot], ring_sem.at[slot])

    wo_copy = pltpu.make_async_copy(wo_hbm, wo, wo_sem)
    wd_copy = pltpu.make_async_copy(wd_hbm, wd, wd_sem)

    x_copy(0).start()
    w_copy(wv_hbm, 0, 0).start()
    w_copy(wv_hbm, 1, 1).start()
    for b in range(1, n_rblk):
        x_copy(b).start()
    w_copy(wk_hbm, 0, 2).start()
    w_copy(wk_hbm, 1, 3).start()
    for j in range(4):
        w_copy(wq_hbm, j, 4 + j).start()
    wo_copy.start()
    wd_copy.start()

    barrier = pltpu.get_barrier_semaphore()
    pl.semaphore_signal(barrier, inc=1, device_id={"tp": 1 - tp}, device_id_type=MESH)
    pl.semaphore_signal(barrier, inc=1, device_id={"cp": partner}, device_id_type=MESH)
    pl.semaphore_signal(barrier, inc=1, device_id={"cp": across}, device_id_type=MESH)

    def region(owner, kind, b):
        if kind:
            at = pl.ds(pl.multiple_of(owner * rows + (b % 2) * (rows // 2), RBLK), rows // 2)
            return k_all.at[at, pl.ds(pl.multiple_of((b // 2) * WBLK, WBLK), WBLK)]
        return vt_all.at[:, pl.ds(pl.multiple_of(owner * rows + b * RBLK, RBLK), RBLK)]

    def kv_copy(owner, kind, b, sends, recvs, target):
        ref = region(owner, kind, b)
        i = kind * n_rblk + b
        return pltpu.make_async_remote_copy(ref, ref, sends.at[i], recvs.at[i], device_id={"cp": target}, device_id_type=MESH)

    def cross(owner, kind, b):
        return kv_copy(owner, kind, b, cross_send, cross_recv, (owner + 2) % 4)

    def up(owner, kind, b):
        return kv_copy(owner, kind, b, up_send, up_recv, (owner + 1) % 4)

    def relay(owner, kind, b):
        return kv_copy(owner, kind, b, relay_send, relay_recv, 3 - owner)

    def send_piece(kind, b):
        @pl.when(me < 2)
        def _():
            cross(me, kind, b).start()

        @pl.when(odd == 0)
        def _():
            up(me, kind, b).start()

    def relay_piece(kind, b):
        owner = me - 2
        cross(owner, kind, b).wait_recv()
        kv_copy(owner, kind, b, relay_send, relay_recv, partner).start()

    def part_copy(c):
        r = pl.ds(pl.multiple_of(c * CHUNK, CHUNK), CHUNK)
        return pltpu.make_async_remote_copy(part.at[r, :], recv.at[r, :], part_send.at[c], part_recv.at[c],
                                            device_id={"tp": 1 - tp}, device_id_type=MESH)

    def via_copy(leg, i):
        n = CHUNK // VIA_PIECES
        rows_i = slice(i * n, (i + 1) * n)
        at = slice(VIA * CHUNK + i * n, VIA * CHUNK + (i + 1) * n)
        src = (part.at[at, :], via.at[0, rows_i, :], via.at[1, rows_i, :])[leg]
        dst = (via.at[0, rows_i, :], via.at[1, rows_i, :], recv.at[at, :])[leg]
        target = {"tp": 1 - tp} if leg == 1 else {"cp": across}
        return pltpu.make_async_remote_copy(src, dst, via_send.at[leg * VIA_PIECES + i], via_recv.at[leg * VIA_PIECES + i],
                                            device_id=target, device_id_type=MESH)

    gain = jnp.concatenate([gain_ref[i:i + 1, :] for i in range(width // HEAD_DIM)], axis=1).astype(F32)

    def norm(b):
        r = pl.ds(pl.multiple_of(b * RBLK, RBLK), RBLK)
        x = x_buf[r, :].astype(F32)
        mean = jnp.mean(x, axis=-1, keepdims=True)
        cent = x - mean
        var = jnp.mean(cent * cent, axis=-1, keepdims=True)
        h_buf[r, :] = (cent * lax.rsqrt(var + LN_EPS) * gain).astype(BF16)

    def project_v(b):
        r = pl.ds(pl.multiple_of(b * RBLK, RBLK), RBLK)
        at = pl.ds(pl.multiple_of(me * rows + b * RBLK, RBLK), RBLK)
        h = h_buf[r, :]
        for j in range(2):
            v = jnp.dot(h, ring[j], preferred_element_type=F32).astype(BF16)
            v_own[r, j * WBLK:(j + 1) * WBLK] = v
            vt_all[j * WBLK:(j + 1) * WBLK, at] = v.T

    x_copy(0).wait()
    norm(0)
    w_copy(wv_hbm, 0, 0).wait()
    w_copy(wv_hbm, 1, 1).wait()
    pl.semaphore_wait(barrier, 3)

    @pl.loop(0, n_rblk - 1)
    def _(b):
        x_copy(b + 1).wait()
        project_v(b)
        norm(b + 1)
        send_piece(0, b)

    project_v(n_rblk - 1)
    send_piece(0, n_rblk - 1)
    v_out = pltpu.make_async_copy(v_own, v_hbm, kv_sem.at[0])
    v_out.start()

    lane = lax.broadcasted_iota(jnp.int32, (WBLK, WBLK), 0)
    other = lax.broadcasted_iota(jnp.int32, (WBLK, WBLK), 1)
    swap = jnp.where(lane == other + 1 - 2 * (other % 2), 1.0, 0.0).astype(BF16)

    def rope_block(slot, dst, row0, col):
        proj = [None] * n_rblk

        def project(b):
            proj[b] = jnp.dot(h_buf[b * RBLK:(b + 1) * RBLK, :], ring[slot], preferred_element_type=F32).astype(BF16)

        project(0)
        for b in range(n_rblk):
            if b + 1 < n_rblk:
                project(b + 1)
            r = slice(b * RBLK, (b + 1) * RBLK)
            swapped = jnp.dot(proj[b], swap, preferred_element_type=F32)
            cos = cos_ref[r, :]
            sin = sin_ref[r, :]
            halves = []
            for i in range(WBLK // HEAD_DIM):
                c = slice(i * HEAD_DIM, (i + 1) * HEAD_DIM)
                halves.append((proj[b][:, c].astype(F32) * cos + swapped[:, c] * sin).astype(BF16))
            at = pl.ds(pl.multiple_of(row0 + b * RBLK, RBLK), RBLK)
            dst[at, pl.ds(pl.multiple_of(col, WBLK), WBLK)] = jnp.concatenate(halves, axis=1)

    @pl.loop(0, 2)
    def _(j):
        w_copy(wk_hbm, j, 2 + j).wait()
        rope_block(2 + j, k_all, me * rows, j * WBLK)
        send_piece(1, 2 * j)
        send_piece(1, 2 * j + 1)

    k_out = pltpu.make_async_copy(k_all.at[pl.ds(pl.multiple_of(me * rows, RBLK), rows), :], k_hbm, kv_sem.at[1])
    k_out.start()

    def ff_copies(s):
        slot = 2 * (s % 4)
        return w_copy(wg_hbm, s % n_ff, slot), w_copy(wu_hbm, s % n_ff, slot + 1)

    for s in range(2):
        for copy in ff_copies(s):
            copy.start()

    @pl.loop(0, 4)
    def _(j):
        w_copy(wq_hbm, j, 4 + j).wait()
        rope_block(4 + j, q_buf, 0, j * WBLK)

    for s in range(2, 4):
        for copy in ff_copies(s):
            copy.start()

    relay_steps = ((0, 0, 0), (2, 0, 1), (6, 0, 2), (10, 0, 3), (15, 1, 0), (19, 1, 1), (23, 1, 2))

    def feed(half):
        @pl.loop(half * n_ff, (half + 1) * n_ff)
        def _(s):
            for copy in ff_copies(s):
                copy.wait()
            slot = 2 * (s % 4)
            for b in range(half * n_rblk // 2, (half + 1) * n_rblk // 2):
                r = slice(b * RBLK, (b + 1) * RBLK)
                h = h_buf[r, :]
                gate = jnp.dot(h, ring[slot], preferred_element_type=F32).astype(BF16).astype(F32)
                up_ = jnp.dot(h, ring[slot + 1], preferred_element_type=F32).astype(BF16).astype(F32)
                act[r, pl.ds(pl.multiple_of((s % n_ff) * WBLK, WBLK), WBLK)] = (jax.nn.silu(gate) * up_).astype(BF16)

            @pl.when(s + 4 < 2 * n_ff)
            def _():
                for copy in ff_copies(s + 4):
                    copy.start()

            for step, kind, b in relay_steps:
                if half * n_ff <= step < (half + 1) * n_ff:
                    @pl.when((me >= 2) & (s == step))
                    def _():
                        relay_piece(kind, b)

    def down(c):
        r = pl.ds(pl.multiple_of(c * CHUNK, CHUNK), CHUNK)
        a = act[r, :]
        for j in range(4):
            cols = slice(j * (width // 4), (j + 1) * (width // 4))
            mlp[:, cols] = jnp.dot(a, wd[:, cols], preferred_element_type=F32)

    scale = HEAD_DIM ** -0.5 * math.log2(math.e)

    def head(g):
        return slice(g * HEAD_DIM, (g + 1) * HEAD_DIM)

    def key_rows(j):
        return pl.ds(pl.multiple_of(j * KEYS, KEYS), KEYS)

    def score(j, g):
        s = lax.dot_general(k_all[key_rows(j), head(g)], qs[g], (((1,), (1,)), ((), ())), preferred_element_type=F32)
        s_ref[g] = s
        blk_ref[g] = jnp.max(s, axis=0, keepdims=True)

    def weigh(g, s, block_top):
        old = top_ref[g]
        new = jnp.maximum(old, block_top)
        factor = jnp.exp2((old - new) * scale)
        weight = jnp.exp2((s - new) * scale)
        top_ref[g] = new
        sum_ref[g] = sum_ref[g] * factor + jnp.sum(weight, axis=0, keepdims=True)
        return factor, weight.astype(BF16)

    def collect(j, g, factor, weight):
        acc_ref[g] = acc_ref[g] * factor + jnp.dot(vt_all[head(g), key_rows(j)], weight, preferred_element_type=F32)

    def chunk(c, stop):
        r = pl.ds(pl.multiple_of(c * CHUNK, CHUNK), CHUNK)
        for g in range(kv_heads):
            for i in range(2):
                col = (2 * g + i) * HEAD_DIM
                qs[g, i * CHUNK:(i + 1) * CHUNK, :] = q_buf[r, col:col + HEAD_DIM]
        top_ref[...] = jnp.full_like(top_ref, -jnp.inf)
        sum_ref[...] = jnp.zeros_like(sum_ref)
        acc_ref[...] = jnp.zeros_like(acc_ref)
        full = me * (rows // KEYS) + c // (KEYS // CHUNK)
        for g in range(kv_heads):
            score(0, g)

        @pl.loop(0, full)
        def _(j):
            for g in range(kv_heads):
                factor, weight = weigh(g, s_ref[g], blk_ref[g])
                score(j + 1, g)
                collect(j, g, factor, weight)

        first = (c % (KEYS // CHUNK)) * CHUNK
        key_id = lax.broadcasted_iota(jnp.int32, (KEYS, 2 * CHUNK), 0)
        query_id = lax.broadcasted_iota(jnp.int32, (KEYS, 2 * CHUNK), 1) % CHUNK
        for g in range(kv_heads):
            s = jnp.where(key_id <= query_id + first, s_ref[g], -jnp.inf)
            factor, weight = weigh(g, s, jnp.max(s, axis=0, keepdims=True))
            collect(full, g, factor, weight)
        for g in range(kv_heads):
            o = (acc_ref[g] / sum_ref[g]).T.astype(BF16)
            for i in range(2):
                col = (2 * g + i) * HEAD_DIM
                o_buf[:, col:col + HEAD_DIM] = o[i * CHUNK:(i + 1) * CHUNK, :]
        o = o_buf[...]
        for j in range(4):
            cols = slice(j * (width // 4), (j + 1) * (width // 4))
            part[r, cols] = (jnp.dot(o, wo[:, cols], preferred_element_type=F32) + mlp[:, cols]).astype(BF16)

        @pl.when((me < 2) | (c != VIA))
        def _():
            part_copy(c).start()

        @pl.when((me >= 2) & (c == VIA))
        def _():
            for i in range(VIA_PIECES):
                via_copy(0, i).start()

        @pl.when((me < 2) & (c == VIA_AFTER))
        def _():
            for i in range(VIA_PIECES):
                via_copy(0, i).wait_recv()
                via_copy(1, i).start()

        @pl.when(c + 1 < stop)
        def _():
            down(c + 1)

    early = jnp.where(me < 2, n_chunk // 2, 0)
    feed(0)
    wo_copy.wait()
    wd_copy.wait()

    @pl.when(odd == 1)
    def _():
        for kind in range(2):
            for b in range(n_rblk):
                up(me - 1, kind, b).wait_recv()

    @pl.when(me < 2)
    def _():
        down(0)

    @pl.loop(0, early)
    def _(c):
        chunk(c, early)

    feed(1)
    down(early)

    @pl.when(me >= 2)
    def _():
        relay_piece(1, 3)
        for kind in range(2):
            for b in range(n_rblk):
                kv_copy(3 - me, kind, b, relay_send, relay_recv, partner).wait_recv()

    @pl.loop(early, n_chunk)
    def _(c):
        chunk(c, n_chunk)

    def out_copy(c):
        r = pl.ds(pl.multiple_of(c * CHUNK, CHUNK), CHUNK)
        return pltpu.make_async_copy(x_buf.at[r, :], out_hbm.at[r, :], out_sem.at[c])

    def finish(c):
        r = pl.ds(pl.multiple_of(c * CHUNK, CHUNK), CHUNK)
        x_buf[r, :] = (x_buf[r, :].astype(F32) + (part[r, :].astype(F32) + recv[r, :].astype(F32))).astype(BF16)
        out_copy(c).start()

    @pl.loop(0, n_chunk)
    def _(c):
        @pl.when((me < 2) & (c == VIA_AFTER + 1))
        def _():
            for i in range(VIA_PIECES):
                via_copy(1, i).wait_recv()
                via_copy(2, i).start()

        @pl.when((me >= 2) & (c == n_chunk - 1))
        def _():
            for i in range(VIA_PIECES):
                via_copy(2, i).wait_recv()
            finish(VIA)

        @pl.when((me < 2) | (c != VIA))
        def _():
            part_copy(c).wait_recv()
            finish(c)

    @pl.loop(0, n_chunk)
    def _(c):
        out_copy(c).wait()

        @pl.when((me < 2) | (c != VIA))
        def _():
            part_copy(c).wait_send()

    for i in range(VIA_PIECES):
        @pl.when(me >= 2)
        def _():
            via_copy(0, i).wait_send()

        @pl.when(me < 2)
        def _():
            via_copy(1, i).wait_send()
            via_copy(2, i).wait_send()

    v_out.wait()
    k_out.wait()
    for kind in range(2):
        for b in range(n_rblk):
            @pl.when(me < 2)
            def _():
                cross(me, kind, b).wait_send()

            @pl.when(odd == 0)
            def _():
                up(me, kind, b).wait_send()

            @pl.when(me >= 2)
            def _():
                kv_copy(me - 2, kind, b, relay_send, relay_recv, partner).wait_send()


def rope_tables(positions):
    lane = jnp.arange(HEAD_DIM)
    exponent = (lane - lane % 2).astype(F32) / HEAD_DIM
    inv_freq = 1.0 / (ROPE_BASE ** exponent)
    angles = positions.astype(F32)[:, None] * inv_freq[None, :]
    sign = jnp.where(lane % 2 == 0, -1.0, 1.0).astype(F32)
    return jnp.cos(angles), jnp.sin(angles) * sign[None, :]


def solution(mesh):
    n_cp = mesh.shape['cp']

    def local_layer(hidden, positions, ln_gain, w_q, w_k, w_v, w_o, w_gate, w_up, w_down):
        rows, width = hidden.shape
        q_cols = w_q.shape[1]
        kv_cols = w_k.shape[1]
        ff = w_gate.shape[1]
        kv_heads = kv_cols // HEAD_DIM
        keys = n_cp * rows
        n_chunk = rows // CHUNK
        pieces = 2 * (rows // RBLK)
        cos, sin = rope_tables(positions)
        hbm = pl.BlockSpec(memory_space=pl.ANY)
        vmem = pl.BlockSpec(memory_space=pltpu.VMEM)
        dma = pltpu.SemaphoreType.DMA
        out, k, v = pl.pallas_call(
            layer_kernel,
            in_specs=[hbm, vmem, vmem, vmem] + [hbm] * 7,
            out_specs=[hbm] * 3,
            out_shape=[
                jax.ShapeDtypeStruct((rows, width), BF16),
                jax.ShapeDtypeStruct((rows, kv_cols), BF16),
                jax.ShapeDtypeStruct((rows, kv_cols), BF16),
            ],
            scratch_shapes=[
                pltpu.VMEM((rows, width), BF16),
                pltpu.VMEM((rows, width), BF16),
                pltpu.VMEM((RING, width, WBLK), BF16),
                pltpu.VMEM((rows, ff), BF16),
                pltpu.VMEM((rows, q_cols), BF16),
                pltpu.VMEM((keys, kv_cols), BF16),
                pltpu.VMEM((kv_cols, keys), BF16),
                pltpu.VMEM((rows, kv_cols), BF16),
                pltpu.VMEM((q_cols, width), BF16),
                pltpu.VMEM((ff, width), BF16),
                pltpu.VMEM((rows, width), BF16),
                pltpu.VMEM((CHUNK, width), F32),
                pltpu.VMEM((kv_heads, 2 * CHUNK, HEAD_DIM), BF16),
                pltpu.VMEM((CHUNK, q_cols), BF16),
                pltpu.VMEM((kv_heads, KEYS, 2 * CHUNK), F32),
                pltpu.VMEM((kv_heads, 1, 2 * CHUNK), F32),
                pltpu.VMEM((kv_heads, 1, 2 * CHUNK), F32),
                pltpu.VMEM((kv_heads, 1, 2 * CHUNK), F32),
                pltpu.VMEM((kv_heads, HEAD_DIM, 2 * CHUNK), F32),
                dma((rows // RBLK,)), dma((RING,)), dma, dma, dma((2,)), dma((n_chunk,)),
                dma((pieces,)), dma((pieces,)), dma((pieces,)), dma((pieces,)), dma((pieces,)), dma((pieces,)),
                dma((n_chunk,)), dma((n_chunk,)),
                pltpu.VMEM((2, CHUNK, width), BF16), dma((3 * VIA_PIECES,)), dma((3 * VIA_PIECES,)),
            ],
            compiler_params=pltpu.CompilerParams(collective_id=0, has_side_effects=True, vmem_limit_bytes=VMEM_LIMIT),
            name="layer",
        )(hidden, ln_gain.reshape(width // HEAD_DIM, HEAD_DIM), cos, sin, w_q, w_k, w_v, w_o, w_gate, w_up, w_down)
        shape = (rows, kv_heads, HEAD_DIM)
        return out, k.reshape(shape), v.reshape(shape)

    row_spec = P(('dp', 'cp'), None)
    col_spec = P(None, 'tp')
    cache_spec = P(('dp', 'cp'), 'tp', None)
    in_specs = (row_spec, P(('dp', 'cp')), P(None), col_spec, col_spec, col_spec, P('tp', None), col_spec, col_spec, P('tp', None))
    return jax.shard_map(local_layer, mesh=mesh, in_specs=in_specs, out_specs=(row_spec, cache_spec, cache_spec), check_vma=False)
```

```python
import functools
import math

import jax
import jax.numpy as jnp
import numpy as np
from jax import lax
from jax.experimental import pallas as pl
from jax.experimental.pallas import tpu as pltpu
from jax.sharding import PartitionSpec as P

HEAD_DIM = 128
ROPE_BASE = 4000000
LN_EPS = 1e-5
F32 = jnp.float32
BF16 = jnp.bfloat16
MESH = pl.DeviceIdType.MESH
VMEM_LIMIT = 67043328

WBLK = 256
RING = 8
RBLK = 256
CHUNK = 128
KEYS = 512
VIA = 2
VIA_AFTER = 6
VIA_PIECES = 4


def layer_kernel(x_hbm, gain_ref, pos_ref, freq_ref, wq_hbm, wk_hbm, wv_hbm, wo_hbm, wg_hbm, wu_hbm, wd_hbm,
                 out_hbm, k_hbm, v_hbm,
                 x_buf, h_buf, ring, act, q_buf, k_all, vt_all, v_own, wo, wd, recv, mlp, qs, o_buf, s_ref, blk_ref, top_ref, sum_ref, acc_ref,
                 x_sem, ring_sem, wo_sem, wd_sem, kv_sem, out_sem,
                 cross_send, cross_recv, up_send, up_recv, relay_send, relay_recv, part_send, part_recv, via, via_send, via_recv, cos_ref, sin_ref, swap):
    me = lax.axis_index("cp")
    tp = lax.axis_index("tp")
    odd = me % 2
    partner = me + 1 - 2 * odd
    across = (me + 2) % 4
    rows, width = x_buf.shape
    kv_heads = k_all.shape[1] // HEAD_DIM
    n_rblk = rows // RBLK
    n_chunk = rows // CHUNK
    n_ff = act.shape[1] // WBLK
    part = h_buf

    def x_copy(b):
        r = pl.ds(pl.multiple_of(b * RBLK, RBLK), RBLK)
        return pltpu.make_async_copy(x_hbm.at[r, :], x_buf.at[r, :], x_sem.at[b])

    def w_copy(w_hbm, blk, slot):
        c = pl.ds(pl.multiple_of(blk * WBLK, WBLK), WBLK)
        return pltpu.make_async_copy(w_hbm.at[:, c], ring.at[slot], ring_sem.at[slot])

    wo_copy = pltpu.make_async_copy(wo_hbm, wo, wo_sem)
    wd_copy = pltpu.make_async_copy(wd_hbm, wd, wd_sem)

    x_copy(0).start()
    w_copy(wv_hbm, 0, 0).start()
    w_copy(wv_hbm, 1, 1).start()
    for b in range(1, n_rblk):
        x_copy(b).start()
    for j in range(4):
        w_copy(wq_hbm, j, 4 + j).start()
    w_copy(wk_hbm, 0, 2).start()
    w_copy(wk_hbm, 1, 3).start()
    wo_copy.start()
    wd_copy.start()

    barrier = pltpu.get_barrier_semaphore()
    pl.semaphore_signal(barrier, inc=1, device_id={"tp": 1 - tp}, device_id_type=MESH)
    pl.semaphore_signal(barrier, inc=1, device_id={"cp": partner}, device_id_type=MESH)
    pl.semaphore_signal(barrier, inc=1, device_id={"cp": across}, device_id_type=MESH)

    def region(owner, kind, b):
        if kind:
            at = pl.ds(pl.multiple_of(owner * rows + (b % 2) * (rows // 2), RBLK), rows // 2)
            return k_all.at[at, pl.ds(pl.multiple_of((b // 2) * WBLK, WBLK), WBLK)]
        return vt_all.at[:, pl.ds(pl.multiple_of(owner * rows + b * RBLK, RBLK), RBLK)]

    def kv_copy(owner, kind, b, sends, recvs, target):
        ref = region(owner, kind, b)
        i = kind * n_rblk + b
        return pltpu.make_async_remote_copy(ref, ref, sends.at[i], recvs.at[i], device_id={"cp": target}, device_id_type=MESH)

    def cross(owner, kind, b):
        return kv_copy(owner, kind, b, cross_send, cross_recv, (owner + 2) % 4)

    def up(owner, kind, b):
        return kv_copy(owner, kind, b, up_send, up_recv, (owner + 1) % 4)

    def relay(owner, kind, b):
        return kv_copy(owner, kind, b, relay_send, relay_recv, 3 - owner)

    def send_piece(kind, b):
        @pl.when(me < 2)
        def _():
            cross(me, kind, b).start()

        @pl.when(odd == 0)
        def _():
            up(me, kind, b).start()

    def relay_piece(kind, b):
        owner = me - 2
        cross(owner, kind, b).wait_recv()
        kv_copy(owner, kind, b, relay_send, relay_recv, partner).start()

    def part_copy(c):
        r = pl.ds(pl.multiple_of(c * CHUNK, CHUNK), CHUNK)
        return pltpu.make_async_remote_copy(part.at[r, :], recv.at[r, :], part_send.at[c], part_recv.at[c],
                                            device_id={"tp": 1 - tp}, device_id_type=MESH)

    def via_copy(leg, i):
        n = CHUNK // VIA_PIECES
        rows_i = slice(i * n, (i + 1) * n)
        at = slice(VIA * CHUNK + i * n, VIA * CHUNK + (i + 1) * n)
        src = (part.at[at, :], via.at[0, rows_i, :], via.at[1, rows_i, :])[leg]
        dst = (via.at[0, rows_i, :], via.at[1, rows_i, :], recv.at[at, :])[leg]
        target = {"tp": 1 - tp} if leg == 1 else {"cp": across}
        return pltpu.make_async_remote_copy(src, dst, via_send.at[leg * VIA_PIECES + i], via_recv.at[leg * VIA_PIECES + i],
                                            device_id=target, device_id_type=MESH)

    gain = jnp.concatenate([gain_ref[i:i + 1, :] for i in range(width // HEAD_DIM)], axis=1).astype(F32)

    def norm(b):
        r = pl.ds(pl.multiple_of(b * RBLK, RBLK), RBLK)
        x = x_buf[r, :].astype(F32)
        mean = jnp.mean(x, axis=-1, keepdims=True)
        cent = x - mean
        var = jnp.mean(cent * cent, axis=-1, keepdims=True)
        h_buf[r, :] = (cent * lax.rsqrt(var + LN_EPS) * gain).astype(BF16)

    def project_v(b):
        r = pl.ds(pl.multiple_of(b * RBLK, RBLK), RBLK)
        at = pl.ds(pl.multiple_of(me * rows + b * RBLK, RBLK), RBLK)
        h = h_buf[r, :]
        for j in range(2):
            v = jnp.dot(h, ring[j], preferred_element_type=F32).astype(BF16)
            v_own[b % 2, :, j * WBLK:(j + 1) * WBLK] = v
            vt_all[j * WBLK:(j + 1) * WBLK, at] = v.T

    def v_copy(b):
        r = pl.ds(pl.multiple_of(b * RBLK, RBLK), RBLK)
        return pltpu.make_async_copy(v_own.at[b % 2], v_hbm.at[r, :], kv_sem.at[b % 2])

    x_copy(0).wait()
    norm(0)
    w_copy(wv_hbm, 0, 0).wait()
    w_copy(wv_hbm, 1, 1).wait()
    pl.semaphore_wait(barrier, 3)

    @pl.loop(0, n_rblk - 1)
    def _(b):
        x_copy(b + 1).wait()

        @pl.when(b >= 2)
        def _():
            v_copy(b - 2).wait()

        project_v(b)
        norm(b + 1)
        send_piece(0, b)
        v_copy(b).start()

    v_copy(n_rblk - 3).wait()
    project_v(n_rblk - 1)
    send_piece(0, n_rblk - 1)
    v_copy(n_rblk - 1).start()

    def ff_copies(s):
        slot = 2 * (s % 4)
        return w_copy(wg_hbm, s % n_ff, slot), w_copy(wu_hbm, s % n_ff, slot + 1)

    def ff_start(s):
        for copy in ff_copies(s):
            copy.start()

    ff_start(0)
    sign = jnp.where(lax.broadcasted_iota(jnp.int32, (1, HEAD_DIM), 1) % 2 == 0, -1.0, 1.0).astype(F32)

    @pl.loop(0, 4)
    def _(j):
        w_copy(wq_hbm, j, 4 + j).wait()
        for b in range(n_rblk):
            r = slice(b * RBLK, (b + 1) * RBLK)
            cols = pl.ds(pl.multiple_of(j * WBLK, WBLK), WBLK)
            q_buf[r, cols] = jnp.dot(h_buf[r, :], ring[4 + j], preferred_element_type=F32).astype(BF16)
        for i in range(2):
            row = 2 * j + i
            pos = jnp.broadcast_to(pos_ref[pl.ds(row, 1), :].astype(F32), (HEAD_DIM, HEAD_DIM)).T
            angle = pos * freq_ref[...]
            at = pl.ds(pl.multiple_of(row * HEAD_DIM, HEAD_DIM), HEAD_DIM)
            cos_ref[at, :] = jnp.cos(angle)
            sin_ref[at, :] = jnp.sin(angle) * sign

    ff_start(2)
    ff_start(3)

    lane = lax.broadcasted_iota(jnp.int32, (WBLK, WBLK), 0)
    other = lax.broadcasted_iota(jnp.int32, (WBLK, WBLK), 1)
    swap[...] = jnp.where(lane == other + 1 - 2 * (other % 2), 1.0, 0.0).astype(BF16)

    def rotate(proj, swapped, r):
        cos = cos_ref[r, :]
        sin = sin_ref[r, :]
        heads = [slice(i * HEAD_DIM, (i + 1) * HEAD_DIM) for i in range(WBLK // HEAD_DIM)]
        return [(proj[:, c].astype(F32) * cos + swapped[:, c] * sin).astype(BF16) for c in heads]

    @pl.loop(0, 2)
    def _(j):
        w_copy(wk_hbm, j, 2 + j).wait()
        proj = [None] * n_rblk

        def project(b):
            proj[b] = jnp.dot(h_buf[b * RBLK:(b + 1) * RBLK, :], ring[2 + j], preferred_element_type=F32).astype(BF16)

        project(0)
        for b in range(n_rblk):
            if b + 1 < n_rblk:
                project(b + 1)
            swapped = jnp.dot(proj[b], swap[...], preferred_element_type=F32)
            at = pl.ds(pl.multiple_of(me * rows + b * RBLK, RBLK), RBLK)
            cols = pl.ds(pl.multiple_of(j * WBLK, WBLK), WBLK)
            k_all[at, cols] = jnp.concatenate(rotate(proj[b], swapped, slice(b * RBLK, (b + 1) * RBLK)), axis=1)
        send_piece(1, 2 * j)
        send_piece(1, 2 * j + 1)

    ff_start(1)
    k_out = pltpu.make_async_copy(k_all.at[pl.ds(pl.multiple_of(me * rows, RBLK), rows), :], k_hbm, kv_sem.at[2])
    k_out.start()

    relay_steps = ((12, 0, 0), (14, 0, 1), (18, 0, 2), (22, 0, 3), (27, 1, 0), (31, 1, 1), (35, 1, 2))
    n_steps = 3 * n_ff

    def feed(first_step, first_block, n_blocks):
        @pl.loop(first_step, first_step + n_ff)
        def _(s):
            for copy in ff_copies(s):
                copy.wait()
            slot = 2 * (s % 4)
            for b in range(n_blocks):
                r = pl.ds(pl.multiple_of((first_block + b) * RBLK, RBLK), RBLK)
                h = h_buf[r, :]
                gate = jnp.dot(h, ring[slot], preferred_element_type=F32).astype(BF16).astype(F32)
                up_ = jnp.dot(h, ring[slot + 1], preferred_element_type=F32).astype(BF16).astype(F32)
                act[r, pl.ds(pl.multiple_of((s % n_ff) * WBLK, WBLK), WBLK)] = (jax.nn.silu(gate) * up_).astype(BF16)

            @pl.when(s + 4 < n_steps)
            def _():
                ff_start(s + 4)

            for step, kind, b in relay_steps:
                @pl.when((me >= 2) & (s == step))
                def _():
                    relay_piece(kind, b)

    def down(c):
        r = pl.ds(pl.multiple_of(c * CHUNK, CHUNK), CHUNK)
        a = act[r, :]
        for j in range(4):
            cols = slice(j * (width // 4), (j + 1) * (width // 4))
            mlp[:, cols] = jnp.dot(a, wd[:, cols], preferred_element_type=F32)

    scale = HEAD_DIM ** -0.5 * math.log2(math.e)

    def head(g):
        return slice(g * HEAD_DIM, (g + 1) * HEAD_DIM)

    def key_rows(j):
        return pl.ds(pl.multiple_of(j * KEYS, KEYS), KEYS)

    def score(j, g):
        s = lax.dot_general(k_all[key_rows(j), head(g)], qs[g], (((1,), (1,)), ((), ())), preferred_element_type=F32)
        s_ref[g] = s
        blk_ref[g] = jnp.max(s, axis=0, keepdims=True)

    def weigh(g, s, block_top):
        old = top_ref[g]
        new = jnp.maximum(old, block_top)
        factor = jnp.exp2((old - new) * scale)
        weight = jnp.exp2((s - new) * scale)
        top_ref[g] = new
        sum_ref[g] = sum_ref[g] * factor + jnp.sum(weight, axis=0, keepdims=True)
        return factor, weight.astype(BF16)

    def collect(j, g, factor, weight):
        acc_ref[g] = acc_ref[g] * factor + jnp.dot(vt_all[head(g), key_rows(j)], weight, preferred_element_type=F32)

    def chunk(c, stop):
        r = pl.ds(pl.multiple_of(c * CHUNK, CHUNK), CHUNK)
        swapped = [jnp.dot(q_buf[r, g * WBLK:(g + 1) * WBLK], swap[...], preferred_element_type=F32) for g in range(kv_heads)]
        for g in range(kv_heads):
            for i, q in enumerate(rotate(q_buf[r, g * WBLK:(g + 1) * WBLK], swapped[g], r)):
                qs[g, i * CHUNK:(i + 1) * CHUNK, :] = q
        top_ref[...] = jnp.full_like(top_ref, -jnp.inf)
        sum_ref[...] = jnp.zeros_like(sum_ref)
        acc_ref[...] = jnp.zeros_like(acc_ref)
        full = me * (rows // KEYS) + c // (KEYS // CHUNK)
        for g in range(kv_heads):
            score(0, g)

        @pl.loop(0, full)
        def _(j):
            for g in range(kv_heads):
                factor, weight = weigh(g, s_ref[g], blk_ref[g])
                score(j + 1, g)
                collect(j, g, factor, weight)

        first = (c % (KEYS // CHUNK)) * CHUNK
        key_id = lax.broadcasted_iota(jnp.int32, (KEYS, 2 * CHUNK), 0)
        query_id = lax.broadcasted_iota(jnp.int32, (KEYS, 2 * CHUNK), 1) % CHUNK
        for g in range(kv_heads):
            s = jnp.where(key_id <= query_id + first, s_ref[g], -jnp.inf)
            factor, weight = weigh(g, s, jnp.max(s, axis=0, keepdims=True))
            collect(full, g, factor, weight)
        for g in range(kv_heads):
            o = (acc_ref[g] / sum_ref[g]).T.astype(BF16)
            for i in range(2):
                col = (2 * g + i) * HEAD_DIM
                o_buf[:, col:col + HEAD_DIM] = o[i * CHUNK:(i + 1) * CHUNK, :]
        o = o_buf[...]
        for j in range(4):
            cols = slice(j * (width // 4), (j + 1) * (width // 4))
            part[r, cols] = (jnp.dot(o, wo[:, cols], preferred_element_type=F32) + mlp[:, cols]).astype(BF16)

        @pl.when((me < 2) | (c != VIA))
        def _():
            part_copy(c).start()

        @pl.when((me >= 2) & (c == VIA))
        def _():
            for i in range(VIA_PIECES):
                via_copy(0, i).start()

        @pl.when((me < 2) & (c == VIA_AFTER))
        def _():
            for i in range(VIA_PIECES):
                via_copy(0, i).wait_recv()
                via_copy(1, i).start()

        @pl.when(c + 1 < stop)
        def _():
            down(c + 1)

    per_block = RBLK // CHUNK
    early = jnp.where(me < 2, 2, 0)

    def await_weights():
        wo_copy.wait()
        wd_copy.wait()

        @pl.when(odd == 1)
        def _():
            for kind in range(2):
                for b in range(n_rblk):
                    up(me - 1, kind, b).wait_recv()

    @pl.loop(0, early)
    def _(block):
        feed(block * n_ff, block, 1)

        @pl.when(block == 0)
        def _():
            await_weights()

        first = block * per_block
        down(first)

        @pl.loop(first, first + per_block)
        def _(c):
            chunk(c, first + per_block)

    @pl.when(me >= 2)
    def _():
        feed(n_ff, 0, 2)
        await_weights()

    feed(2 * n_ff, 2, 2)
    down(early * per_block)

    @pl.when(me >= 2)
    def _():
        relay_piece(1, 3)
        for kind in range(2):
            for b in range(n_rblk):
                kv_copy(3 - me, kind, b, relay_send, relay_recv, partner).wait_recv()

    @pl.loop(early * per_block, n_chunk)
    def _(c):
        chunk(c, n_chunk)

    def out_copy(c):
        r = pl.ds(pl.multiple_of(c * CHUNK, CHUNK), CHUNK)
        return pltpu.make_async_copy(x_buf.at[r, :], out_hbm.at[r, :], out_sem.at[c])

    def finish(c):
        r = pl.ds(pl.multiple_of(c * CHUNK, CHUNK), CHUNK)
        x_buf[r, :] = (x_buf[r, :].astype(F32) + (part[r, :].astype(F32) + recv[r, :].astype(F32))).astype(BF16)
        out_copy(c).start()

    @pl.loop(0, n_chunk)
    def _(c):
        @pl.when((me < 2) & (c == VIA_AFTER + 1))
        def _():
            for i in range(VIA_PIECES):
                via_copy(1, i).wait_recv()
                via_copy(2, i).start()

        @pl.when((me >= 2) & (c == n_chunk - 1))
        def _():
            for i in range(VIA_PIECES):
                via_copy(2, i).wait_recv()
            finish(VIA)

        @pl.when((me < 2) | (c != VIA))
        def _():
            part_copy(c).wait_recv()
            finish(c)

    @pl.loop(0, n_chunk)
    def _(c):
        out_copy(c).wait()

        @pl.when((me < 2) | (c != VIA))
        def _():
            part_copy(c).wait_send()

    for i in range(VIA_PIECES):
        @pl.when(me >= 2)
        def _():
            via_copy(0, i).wait_send()

        @pl.when(me < 2)
        def _():
            via_copy(1, i).wait_send()
            via_copy(2, i).wait_send()

    v_copy(n_rblk - 2).wait()
    v_copy(n_rblk - 1).wait()
    k_out.wait()
    for kind in range(2):
        for b in range(n_rblk):
            @pl.when(me < 2)
            def _():
                cross(me, kind, b).wait_send()

            @pl.when(odd == 0)
            def _():
                up(me, kind, b).wait_send()

            @pl.when(me >= 2)
            def _():
                kv_copy(me - 2, kind, b, relay_send, relay_recv, partner).wait_send()


def place_kernel(m_ref, k_ref, v_ref, out_ref, kc_ref, vc_ref):
    out_ref[...] = m_ref[...]
    kc_ref[...] = k_ref[...].reshape(kc_ref.shape)
    vc_ref[...] = v_ref[...].reshape(vc_ref.shape)


def place(out, k, v, kv_heads):
    rows, width = out.shape
    blk = 256
    kv_spec = pl.BlockSpec((blk, k.shape[1]), lambda i: (i, 0))
    cache_spec = pl.BlockSpec((blk, kv_heads, HEAD_DIM), lambda i: (i, 0, 0))
    cache = jax.ShapeDtypeStruct((rows, kv_heads, HEAD_DIM), BF16)
    return pl.pallas_call(
        place_kernel,
        grid=(rows // blk,),
        in_specs=[pl.BlockSpec((blk, width), lambda i: (i, 0)), kv_spec, kv_spec],
        out_specs=[pl.BlockSpec((blk, width), lambda i: (i, 0)), cache_spec, cache_spec],
        out_shape=[jax.ShapeDtypeStruct((rows, width), BF16), cache, cache],
        compiler_params=pltpu.CompilerParams(dimension_semantics=("arbitrary",)),
        name="place",
    )(out, k, v)


def solution(mesh):
    n_cp = mesh.shape['cp']

    def local_layer(hidden, positions, ln_gain, w_q, w_k, w_v, w_o, w_gate, w_up, w_down):
        rows, width = hidden.shape
        q_cols = w_q.shape[1]
        kv_cols = w_k.shape[1]
        ff = w_gate.shape[1]
        kv_heads = kv_cols // HEAD_DIM
        keys = n_cp * rows
        n_chunk = rows // CHUNK
        pieces = 2 * (rows // RBLK)
        lane = np.arange(HEAD_DIM)
        inv_freq = (1.0 / ROPE_BASE ** ((lane - lane % 2) / HEAD_DIM)).astype(np.float32)
        hbm = pl.BlockSpec(memory_space=pl.ANY)
        vmem = pl.BlockSpec(memory_space=pltpu.VMEM)
        dma = pltpu.SemaphoreType.DMA
        out, k, v = pl.pallas_call(
            layer_kernel,
            in_specs=[hbm, vmem, vmem, vmem] + [hbm] * 7,
            out_specs=[hbm] * 3,
            out_shape=[
                jax.ShapeDtypeStruct((rows, width), BF16),
                jax.ShapeDtypeStruct((rows, kv_cols), BF16),
                jax.ShapeDtypeStruct((rows, kv_cols), BF16),
            ],
            scratch_shapes=[
                pltpu.VMEM((rows, width), BF16),
                pltpu.VMEM((rows, width), BF16),
                pltpu.VMEM((RING, width, WBLK), BF16),
                pltpu.VMEM((rows, ff), BF16),
                pltpu.VMEM((rows, q_cols), BF16),
                pltpu.VMEM((keys, kv_cols), BF16),
                pltpu.VMEM((kv_cols, keys), BF16),
                pltpu.VMEM((2, RBLK, kv_cols), BF16),
                pltpu.VMEM((q_cols, width), BF16),
                pltpu.VMEM((ff, width), BF16),
                pltpu.VMEM((rows, width), BF16),
                pltpu.VMEM((CHUNK, width), F32),
                pltpu.VMEM((kv_heads, 2 * CHUNK, HEAD_DIM), BF16),
                pltpu.VMEM((CHUNK, q_cols), BF16),
                pltpu.VMEM((kv_heads, KEYS, 2 * CHUNK), F32),
                pltpu.VMEM((kv_heads, 1, 2 * CHUNK), F32),
                pltpu.VMEM((kv_heads, 1, 2 * CHUNK), F32),
                pltpu.VMEM((kv_heads, 1, 2 * CHUNK), F32),
                pltpu.VMEM((kv_heads, HEAD_DIM, 2 * CHUNK), F32),
                dma((rows // RBLK,)), dma((RING,)), dma, dma, dma((3,)), dma((n_chunk,)),
                dma((pieces,)), dma((pieces,)), dma((pieces,)), dma((pieces,)), dma((pieces,)), dma((pieces,)),
                dma((n_chunk,)), dma((n_chunk,)),
                pltpu.VMEM((2, CHUNK, width), BF16), dma((3 * VIA_PIECES,)), dma((3 * VIA_PIECES,)),
                pltpu.VMEM((rows, HEAD_DIM), F32), pltpu.VMEM((rows, HEAD_DIM), F32), pltpu.VMEM((WBLK, WBLK), BF16),
            ],
            compiler_params=pltpu.CompilerParams(collective_id=0, has_side_effects=True, vmem_limit_bytes=VMEM_LIMIT),
            name="layer",
        )(hidden, ln_gain.reshape(width // HEAD_DIM, HEAD_DIM), positions.reshape(rows // HEAD_DIM, HEAD_DIM), jnp.asarray(inv_freq[None, :]), w_q, w_k, w_v, w_o, w_gate, w_up, w_down)
        return place(out, k, v, kv_heads)

    row_spec = P(('dp', 'cp'), None)
    col_spec = P(None, 'tp')
    cache_spec = P(('dp', 'cp'), 'tp', None)
    in_specs = (row_spec, P(('dp', 'cp')), P(None), col_spec, col_spec, col_spec, P('tp', None), col_spec, col_spec, P('tp', None))
    return jax.shard_map(local_layer, mesh=mesh, in_specs=in_specs, out_specs=(row_spec, cache_spec, cache_spec), check_vma=False)
```

```python
import functools
import math

import jax
import jax.numpy as jnp
import numpy as np
from jax import lax
from jax.experimental import pallas as pl
from jax.experimental.pallas import tpu as pltpu
from jax.sharding import PartitionSpec as P

HEAD_DIM = 128
ROPE_BASE = 4000000
LN_EPS = 1e-5
F32 = jnp.float32
BF16 = jnp.bfloat16
MESH = pl.DeviceIdType.MESH
VMEM_LIMIT = 67043328

WBLK = 256
RING = 8
RBLK = 256
VBLK = 128
CHUNK = 128
KEYS = 512
VIA = 3
VIA_EXTRA = 16
VIA_AFTER = 6
VIA_PIECES = 9


def layer_kernel(x_hbm, gain_ref, pos_ref, freq_ref, wq_hbm, wk_hbm, wv_hbm, wo_hbm, wg_hbm, wu_hbm, wd_hbm,
                 out_hbm, k_hbm, v_hbm,
                 x_buf, h_buf, ring, act, q_buf, k_all, vt_all, v_own, wo, wd, recv, mlp, qs, o_buf, s_ref, blk_ref, top_ref, sum_ref, acc_ref,
                 x_sem, ring_sem, wo_sem, wd_sem, kv_sem, out_sem,
                 cross_send, cross_recv, up_send, up_recv, relay_send, relay_recv, part_send, part_recv, via, via_send, via_recv, cos_ref, sin_ref, swap):
    me = lax.axis_index("cp")
    tp = lax.axis_index("tp")
    odd = me % 2
    partner = me + 1 - 2 * odd
    across = (me + 2) % 4
    rows, width = x_buf.shape
    kv_heads = k_all.shape[0]
    n_rblk = rows // RBLK
    n_vblk = rows // VBLK
    n_piece = (n_vblk, kv_heads)
    n_chunk = rows // CHUNK
    n_ff = act.shape[1] // WBLK
    part = h_buf

    def x_copy(b):
        r = pl.ds(pl.multiple_of(b * VBLK, VBLK), VBLK)
        return pltpu.make_async_copy(x_hbm.at[r, :], x_buf.at[r, :], x_sem.at[b])

    def w_copy(w_hbm, blk, slot):
        c = pl.ds(pl.multiple_of(blk * WBLK, WBLK), WBLK)
        return pltpu.make_async_copy(w_hbm.at[:, c], ring.at[slot], ring_sem.at[slot])

    wo_copy = pltpu.make_async_copy(wo_hbm, wo, wo_sem)
    wd_copy = pltpu.make_async_copy(wd_hbm, wd, wd_sem)

    x_copy(0).start()
    w_copy(wv_hbm, 0, 0).start()
    w_copy(wv_hbm, 1, 1).start()
    for b in range(1, n_vblk):
        x_copy(b).start()
    for j in range(4):
        w_copy(wq_hbm, j, 4 + j).start()
    w_copy(wk_hbm, 0, 2).start()
    w_copy(wk_hbm, 1, 3).start()
    wo_copy.start()
    wd_copy.start()

    barrier = pltpu.get_barrier_semaphore()
    pl.semaphore_signal(barrier, inc=1, device_id={"tp": 1 - tp}, device_id_type=MESH)
    pl.semaphore_signal(barrier, inc=1, device_id={"cp": partner}, device_id_type=MESH)
    pl.semaphore_signal(barrier, inc=1, device_id={"cp": across}, device_id_type=MESH)

    def region(owner, kind, b):
        if kind:
            return k_all.at[b, pl.ds(pl.multiple_of(owner * rows, RBLK), rows), :]
        return vt_all.at[owner * n_vblk + b]

    def kv_copy(owner, kind, b, sends, recvs, target):
        ref = region(owner, kind, b)
        i = kind * n_vblk + b
        return pltpu.make_async_remote_copy(ref, ref, sends.at[i], recvs.at[i], device_id={"cp": target}, device_id_type=MESH)

    def cross(owner, kind, b):
        return kv_copy(owner, kind, b, cross_send, cross_recv, (owner + 2) % 4)

    def up(owner, kind, b):
        return kv_copy(owner, kind, b, up_send, up_recv, (owner + 1) % 4)

    def relay(owner, kind, b):
        return kv_copy(owner, kind, b, relay_send, relay_recv, 3 - owner)

    def send_piece(kind, b):
        @pl.when(me < 2)
        def _():
            cross(me, kind, b).start()

        @pl.when(odd == 0)
        def _():
            up(me, kind, b).start()

    def relay_piece(kind, b):
        owner = me - 2
        cross(owner, kind, b).wait_recv()
        kv_copy(owner, kind, b, relay_send, relay_recv, partner).start()

    def part_copy(c, n=CHUNK):
        r = pl.ds(pl.multiple_of(c * CHUNK, CHUNK), n)
        return pltpu.make_async_remote_copy(part.at[r, :], recv.at[r, :], part_send.at[c], part_recv.at[c],
                                            device_id={"tp": 1 - tp}, device_id_type=MESH)

    def for_part(c, act_on):
        upper = me >= 2
        short = upper & (c == VIA - 1)

        @pl.when(short)
        def _():
            act_on(part_copy(VIA - 1, CHUNK - VIA_EXTRA))

        @pl.when(jnp.logical_not(short | (upper & (c == VIA))))
        def _():
            act_on(part_copy(c))

    def via_copy(leg, i):
        n = VIA_EXTRA
        rows_i = slice(i * n, (i + 1) * n)
        at = slice(VIA * CHUNK + (i - 1) * n, VIA * CHUNK + i * n)
        src = (part.at[at, :], via.at[0, rows_i, :], via.at[1, rows_i, :])[leg]
        dst = (via.at[0, rows_i, :], via.at[1, rows_i, :], recv.at[at, :])[leg]
        target = {"tp": 1 - tp} if leg == 1 else {"cp": across}
        return pltpu.make_async_remote_copy(src, dst, via_send.at[leg * VIA_PIECES + i], via_recv.at[leg * VIA_PIECES + i],
                                            device_id=target, device_id_type=MESH)

    gain = jnp.concatenate([gain_ref[i:i + 1, :] for i in range(width // HEAD_DIM)], axis=1).astype(F32)

    def norm(b):
        r = pl.ds(pl.multiple_of(b * VBLK, VBLK), VBLK)
        x = x_buf[r, :].astype(F32)
        mean = jnp.mean(x, axis=-1, keepdims=True)
        cent = x - mean
        var = jnp.mean(cent * cent, axis=-1, keepdims=True)
        h_buf[r, :] = (cent * lax.rsqrt(var + LN_EPS) * gain).astype(BF16)

    def project_v(b):
        r = pl.ds(pl.multiple_of(b * VBLK, VBLK), VBLK)
        h = h_buf[r, :]
        for j in range(2):
            v = jnp.dot(h, ring[j], preferred_element_type=F32).astype(BF16)
            v_own[b % 2, :, j * WBLK:(j + 1) * WBLK] = v
            vt_all[me * n_vblk + b, j * WBLK:(j + 1) * WBLK, :] = v.T

    def v_copy(b):
        r = pl.ds(pl.multiple_of(b * VBLK, VBLK), VBLK)
        return pltpu.make_async_copy(v_own.at[b % 2], v_hbm.at[r, :], kv_sem.at[b % 2])

    x_copy(0).wait()
    norm(0)
    w_copy(wv_hbm, 0, 0).wait()
    w_copy(wv_hbm, 1, 1).wait()
    pl.semaphore_wait(barrier, 3)

    @pl.loop(0, n_vblk - 1)
    def _(b):
        x_copy(b + 1).wait()

        @pl.when(b >= 2)
        def _():
            v_copy(b - 2).wait()

        project_v(b)
        norm(b + 1)
        send_piece(0, b)
        v_copy(b).start()

    v_copy(n_vblk - 3).wait()
    project_v(n_vblk - 1)
    send_piece(0, n_vblk - 1)
    v_copy(n_vblk - 1).start()

    def ff_copies(s):
        slot = 2 * (s % 4)
        return w_copy(wg_hbm, s % n_ff, slot), w_copy(wu_hbm, s % n_ff, slot + 1)

    def ff_start(s):
        for copy in ff_copies(s):
            copy.start()

    ff_start(0)
    sign = jnp.where(lax.broadcasted_iota(jnp.int32, (1, HEAD_DIM), 1) % 2 == 0, -1.0, 1.0).astype(F32)

    @pl.loop(0, 4)
    def _(j):
        w_copy(wq_hbm, j, 4 + j).wait()
        for b in range(n_rblk):
            r = slice(b * RBLK, (b + 1) * RBLK)
            cols = pl.ds(pl.multiple_of(j * WBLK, WBLK), WBLK)
            q_buf[r, cols] = jnp.dot(h_buf[r, :], ring[4 + j], preferred_element_type=F32).astype(BF16)
        for i in range(2):
            row = 2 * j + i
            pos = jnp.broadcast_to(pos_ref[pl.ds(row, 1), :].astype(F32), (HEAD_DIM, HEAD_DIM)).T
            angle = pos * freq_ref[...]
            at = pl.ds(pl.multiple_of(row * HEAD_DIM, HEAD_DIM), HEAD_DIM)
            cos_ref[at, :] = jnp.cos(angle)
            sin_ref[at, :] = jnp.sin(angle) * sign

    ff_start(2)
    ff_start(3)

    lane = lax.broadcasted_iota(jnp.int32, (WBLK, WBLK), 0)
    other = lax.broadcasted_iota(jnp.int32, (WBLK, WBLK), 1)
    swap[...] = jnp.where(lane == other + 1 - 2 * (other % 2), 1.0, 0.0).astype(BF16)

    def rotate(proj, swapped, r):
        cos = cos_ref[r, :]
        sin = sin_ref[r, :]
        heads = [slice(i * HEAD_DIM, (i + 1) * HEAD_DIM) for i in range(WBLK // HEAD_DIM)]
        return [(proj[:, c].astype(F32) * cos + swapped[:, c] * sin).astype(BF16) for c in heads]

    @pl.loop(0, 2)
    def _(j):
        w_copy(wk_hbm, j, 2 + j).wait()
        proj = [None] * n_rblk

        def project(b):
            proj[b] = jnp.dot(h_buf[b * RBLK:(b + 1) * RBLK, :], ring[2 + j], preferred_element_type=F32).astype(BF16)

        project(0)
        for b in range(n_rblk):
            if b + 1 < n_rblk:
                project(b + 1)
            swapped = jnp.dot(proj[b], swap[...], preferred_element_type=F32)
            at = pl.ds(pl.multiple_of(me * rows + b * RBLK, RBLK), RBLK)
            for i, k in enumerate(rotate(proj[b], swapped, slice(b * RBLK, (b + 1) * RBLK))):
                k_all[2 * j + i, at, :] = k
        send_piece(1, 2 * j)
        send_piece(1, 2 * j + 1)

    ff_start(1)
    def k_copy(g):
        return pltpu.make_async_copy(k_all.at[g, pl.ds(pl.multiple_of(me * rows, RBLK), rows), :],
                                     k_hbm.at[:, g * HEAD_DIM:(g + 1) * HEAD_DIM], kv_sem.at[2 + g])

    for g in range(kv_heads):
        k_copy(g).start()

    relay_steps = ((12, 0, 0), (12, 0, 1), (12, 0, 2), (12, 0, 3), (14, 0, 4), (16, 0, 5), (19, 0, 6), (21, 0, 7),
                   (26, 1, 0), (30, 1, 1), (34, 1, 2))
    n_steps = 3 * n_ff

    def feed(first_step, first_block, n_blocks):
        @pl.loop(first_step, first_step + n_ff)
        def _(s):
            for copy in ff_copies(s):
                copy.wait()
            slot = 2 * (s % 4)
            for b in range(n_blocks):
                r = pl.ds(pl.multiple_of((first_block + b) * RBLK, RBLK), RBLK)
                h = h_buf[r, :]
                gate = jnp.dot(h, ring[slot], preferred_element_type=F32).astype(BF16).astype(F32)
                up_ = jnp.dot(h, ring[slot + 1], preferred_element_type=F32).astype(BF16).astype(F32)
                act[r, pl.ds(pl.multiple_of((s % n_ff) * WBLK, WBLK), WBLK)] = (jax.nn.silu(gate) * up_).astype(BF16)

            @pl.when(s + 4 < n_steps)
            def _():
                ff_start(s + 4)

            for step, kind, b in relay_steps:
                @pl.when((me >= 2) & (s == step))
                def _():
                    relay_piece(kind, b)

    def down(c):
        r = pl.ds(pl.multiple_of(c * CHUNK, CHUNK), CHUNK)
        a = act[r, :]
        for j in range(4):
            cols = slice(j * (width // 4), (j + 1) * (width // 4))
            mlp[:, cols] = jnp.dot(a, wd[:, cols], preferred_element_type=F32)

    scale = HEAD_DIM ** -0.5 * math.log2(math.e)

    low = jnp.where(me < 2, 0, 2 * (rows // KEYS))

    def head(g):
        return slice(g * HEAD_DIM, (g + 1) * HEAD_DIM)

    def key_rows(j):
        return pl.ds(pl.multiple_of(j * KEYS, KEYS), KEYS)

    def score(j, g):
        s = lax.dot_general(k_all[g, key_rows(j), :], qs[g], (((1,), (1,)), ((), ())), preferred_element_type=F32)
        s_ref[g] = s
        blk_ref[g] = jnp.max(s, axis=0, keepdims=True)

    def weigh(g, s, block_top):
        old = top_ref[g]
        new = jnp.maximum(old, block_top)
        factor = jnp.exp2((old - new) * scale)
        weight = jnp.exp2((s - new) * scale)
        top_ref[g] = new
        sum_ref[g] = sum_ref[g] * factor + jnp.sum(weight, axis=0, keepdims=True)
        return factor, weight.astype(BF16)

    def collect(j, g, factor, weight):
        vt = jnp.concatenate([vt_all[j * (KEYS // VBLK) + i, head(g), :] for i in range(KEYS // VBLK)], axis=1)
        acc_ref[g] = acc_ref[g] * factor + jnp.dot(vt, weight, preferred_element_type=F32)

    def chunk(c, stop):
        r = pl.ds(pl.multiple_of(c * CHUNK, CHUNK), CHUNK)
        swapped = [jnp.dot(q_buf[r, g * WBLK:(g + 1) * WBLK], swap[...], preferred_element_type=F32) for g in range(kv_heads)]
        for g in range(kv_heads):
            for i, q in enumerate(rotate(q_buf[r, g * WBLK:(g + 1) * WBLK], swapped[g], r)):
                qs[g, i * CHUNK:(i + 1) * CHUNK, :] = q
        top_ref[...] = jnp.full_like(top_ref, -jnp.inf)
        sum_ref[...] = jnp.zeros_like(sum_ref)
        acc_ref[...] = jnp.zeros_like(acc_ref)
        full = me * (rows // KEYS) + c // (KEYS // CHUNK)
        for g in range(kv_heads):
            score(low, g)

        def step(j):
            for g in range(kv_heads):
                factor, weight = weigh(g, s_ref[g], blk_ref[g])
                score(j + 1, g)
                collect(j, g, factor, weight)

        @pl.loop(low, full)
        def _(j):
            step(j)

        first = (c % (KEYS // CHUNK)) * CHUNK
        key_id = lax.broadcasted_iota(jnp.int32, (KEYS, 2 * CHUNK), 0)
        query_id = lax.broadcasted_iota(jnp.int32, (KEYS, 2 * CHUNK), 1) % CHUNK
        for g in range(kv_heads):
            s = jnp.where(key_id <= query_id + first, s_ref[g], -jnp.inf)
            factor, weight = weigh(g, s, jnp.max(s, axis=0, keepdims=True))
            collect(full, g, factor, weight)

        @pl.when(me >= 2)
        def _():
            @pl.when(c == 0)
            def _():
                relay_piece(1, 3)
                for kind in range(2):
                    for b in range(n_piece[kind]):
                        kv_copy(3 - me, kind, b, relay_send, relay_recv, partner).wait_recv()

            for g in range(kv_heads):
                score(0, g)

            @pl.loop(0, low)
            def _(j):
                step(j)

        for g in range(kv_heads):
            o = (acc_ref[g] / sum_ref[g]).T.astype(BF16)
            for i in range(2):
                col = (2 * g + i) * HEAD_DIM
                o_buf[:, col:col + HEAD_DIM] = o[i * CHUNK:(i + 1) * CHUNK, :]
        o = o_buf[...]
        for j in range(4):
            cols = slice(j * (width // 4), (j + 1) * (width // 4))
            part[r, cols] = (jnp.dot(o, wo[:, cols], preferred_element_type=F32) + mlp[:, cols]).astype(BF16)

        for_part(c, lambda copy: copy.start())

        @pl.when((me >= 2) & (c == VIA - 1))
        def _():
            via_copy(0, 0).start()

        @pl.when((me >= 2) & (c == VIA))
        def _():
            for i in range(1, VIA_PIECES):
                via_copy(0, i).start()

        @pl.when((me < 2) & (c == VIA_AFTER))
        def _():
            for i in range(VIA_PIECES):
                via_copy(0, i).wait_recv()
                via_copy(1, i).start()

        @pl.when(c + 1 < stop)
        def _():
            down(c + 1)

    per_block = RBLK // CHUNK
    early = jnp.where(me < 2, 2, 0)

    def await_weights():
        wo_copy.wait()
        wd_copy.wait()

        @pl.when(odd == 1)
        def _():
            for kind in range(2):
                for b in range(n_piece[kind]):
                    up(me - 1, kind, b).wait_recv()

    @pl.loop(0, early)
    def _(block):
        feed(block * n_ff, block, 1)

        @pl.when(block == 0)
        def _():
            await_weights()

        first = block * per_block
        down(first)

        @pl.loop(first, first + per_block)
        def _(c):
            chunk(c, first + per_block)

    @pl.when(me >= 2)
    def _():
        feed(n_ff, 0, 2)
        await_weights()

    feed(2 * n_ff, 2, 2)
    down(early * per_block)

    @pl.loop(early * per_block, n_chunk)
    def _(c):
        chunk(c, n_chunk)

    def out_copy(c):
        r = pl.ds(pl.multiple_of(c * CHUNK, CHUNK), CHUNK)
        return pltpu.make_async_copy(x_buf.at[r, :], out_hbm.at[r, :], out_sem.at[c])

    def finish(c):
        r = pl.ds(pl.multiple_of(c * CHUNK, CHUNK), CHUNK)
        x_buf[r, :] = (x_buf[r, :].astype(F32) + (part[r, :].astype(F32) + recv[r, :].astype(F32))).astype(BF16)
        out_copy(c).start()

    @pl.loop(0, n_chunk)
    def _(c):
        @pl.when((me < 2) & (c == VIA_AFTER + 1))
        def _():
            for i in range(VIA_PIECES):
                via_copy(1, i).wait_recv()
                via_copy(2, i).start()

        @pl.when((me >= 2) & (c == n_chunk - 1))
        def _():
            for i in range(VIA_PIECES):
                via_copy(2, i).wait_recv()
            finish(VIA - 1)
            finish(VIA)

        for_part(c, lambda copy: copy.wait_recv())

        @pl.when((me < 2) | ((c != VIA) & (c != VIA - 1)))
        def _():
            finish(c)

    @pl.loop(0, n_chunk)
    def _(c):
        out_copy(c).wait()

        for_part(c, lambda copy: copy.wait_send())

    for i in range(VIA_PIECES):
        @pl.when(me >= 2)
        def _():
            via_copy(0, i).wait_send()

        @pl.when(me < 2)
        def _():
            via_copy(1, i).wait_send()
            via_copy(2, i).wait_send()

    v_copy(n_vblk - 2).wait()
    v_copy(n_vblk - 1).wait()
    for g in range(kv_heads):
        k_copy(g).wait()
    for kind in range(2):
        for b in range(n_piece[kind]):
            @pl.when(me < 2)
            def _():
                cross(me, kind, b).wait_send()

            @pl.when(odd == 0)
            def _():
                up(me, kind, b).wait_send()

            @pl.when(me >= 2)
            def _():
                kv_copy(me - 2, kind, b, relay_send, relay_recv, partner).wait_send()


def place_kernel(m_ref, k_ref, v_ref, out_ref, kc_ref, vc_ref):
    out_ref[...] = m_ref[...]
    kc_ref[...] = k_ref[...].reshape(kc_ref.shape)
    vc_ref[...] = v_ref[...].reshape(vc_ref.shape)


def place(out, k, v, kv_heads):
    rows, width = out.shape
    blk = 512
    kv_spec = pl.BlockSpec((blk, k.shape[1]), lambda i: (i, 0))
    cache_spec = pl.BlockSpec((blk, kv_heads, HEAD_DIM), lambda i: (i, 0, 0))
    cache = jax.ShapeDtypeStruct((rows, kv_heads, HEAD_DIM), BF16)
    return pl.pallas_call(
        place_kernel,
        grid=(rows // blk,),
        in_specs=[pl.BlockSpec((blk, width), lambda i: (i, 0)), kv_spec, kv_spec],
        out_specs=[pl.BlockSpec((blk, width), lambda i: (i, 0)), cache_spec, cache_spec],
        out_shape=[jax.ShapeDtypeStruct((rows, width), BF16), cache, cache],
        compiler_params=pltpu.CompilerParams(dimension_semantics=("arbitrary",)),
        name="place",
    )(out, k, v)


def solution(mesh):
    n_cp = mesh.shape['cp']

    def local_layer(hidden, positions, ln_gain, w_q, w_k, w_v, w_o, w_gate, w_up, w_down):
        rows, width = hidden.shape
        q_cols = w_q.shape[1]
        kv_cols = w_k.shape[1]
        ff = w_gate.shape[1]
        kv_heads = kv_cols // HEAD_DIM
        keys = n_cp * rows
        n_chunk = rows // CHUNK
        pieces = rows // VBLK + kv_heads
        lane = np.arange(HEAD_DIM)
        inv_freq = (1.0 / ROPE_BASE ** ((lane - lane % 2) / HEAD_DIM)).astype(np.float32)
        hbm = pl.BlockSpec(memory_space=pl.ANY)
        vmem = pl.BlockSpec(memory_space=pltpu.VMEM)
        dma = pltpu.SemaphoreType.DMA
        out, k, v = pl.pallas_call(
            layer_kernel,
            in_specs=[hbm, vmem, vmem, vmem] + [hbm] * 7,
            out_specs=[hbm] * 3,
            out_shape=[
                jax.ShapeDtypeStruct((rows, width), BF16),
                jax.ShapeDtypeStruct((rows, kv_cols), BF16),
                jax.ShapeDtypeStruct((rows, kv_cols), BF16),
            ],
            scratch_shapes=[
                pltpu.VMEM((rows, width), BF16),
                pltpu.VMEM((rows, width), BF16),
                pltpu.VMEM((RING, width, WBLK), BF16),
                pltpu.VMEM((rows, ff), BF16),
                pltpu.VMEM((rows, q_cols), BF16),
                pltpu.VMEM((kv_heads, keys, HEAD_DIM), BF16),
                pltpu.VMEM((keys // VBLK, kv_cols, VBLK), BF16),
                pltpu.VMEM((2, VBLK, kv_cols), BF16),
                pltpu.VMEM((q_cols, width), BF16),
                pltpu.VMEM((ff, width), BF16),
                pltpu.VMEM((rows, width), BF16),
                pltpu.VMEM((CHUNK, width), F32),
                pltpu.VMEM((kv_heads, 2 * CHUNK, HEAD_DIM), BF16),
                pltpu.VMEM((CHUNK, q_cols), BF16),
                pltpu.VMEM((kv_heads, KEYS, 2 * CHUNK), F32),
                pltpu.VMEM((kv_heads, 1, 2 * CHUNK), F32),
                pltpu.VMEM((kv_heads, 1, 2 * CHUNK), F32),
                pltpu.VMEM((kv_heads, 1, 2 * CHUNK), F32),
                pltpu.VMEM((kv_heads, HEAD_DIM, 2 * CHUNK), F32),
                dma((rows // VBLK,)), dma((RING,)), dma, dma, dma((2 + kv_heads,)), dma((n_chunk,)),
                dma((pieces,)), dma((pieces,)), dma((pieces,)), dma((pieces,)), dma((pieces,)), dma((pieces,)),
                dma((n_chunk,)), dma((n_chunk,)),
                pltpu.VMEM((2, VIA_EXTRA * VIA_PIECES, width), BF16), dma((3 * VIA_PIECES,)), dma((3 * VIA_PIECES,)),
                pltpu.VMEM((rows, HEAD_DIM), F32), pltpu.VMEM((rows, HEAD_DIM), F32), pltpu.VMEM((WBLK, WBLK), BF16),
            ],
            compiler_params=pltpu.CompilerParams(collective_id=0, has_side_effects=True, vmem_limit_bytes=VMEM_LIMIT),
            name="layer",
        )(hidden, ln_gain.reshape(width // HEAD_DIM, HEAD_DIM), positions.reshape(rows // HEAD_DIM, HEAD_DIM), jnp.asarray(inv_freq[None, :]), w_q, w_k, w_v, w_o, w_gate, w_up, w_down)
        return place(out, k, v, kv_heads)

    row_spec = P(('dp', 'cp'), None)
    col_spec = P(None, 'tp')
    cache_spec = P(('dp', 'cp'), 'tp', None)
    in_specs = (row_spec, P(('dp', 'cp')), P(None), col_spec, col_spec, col_spec, P('tp', None), col_spec, col_spec, P('tp', None))
    return jax.shard_map(local_layer, mesh=mesh, in_specs=in_specs, out_specs=(row_spec, cache_spec, cache_spec), check_vma=False)
```

```python
import functools
import math

import jax
import jax.numpy as jnp
import numpy as np
from jax import lax
from jax.experimental import pallas as pl
from jax.experimental.pallas import tpu as pltpu
from jax.sharding import PartitionSpec as P

HEAD_DIM = 128
ROPE_BASE = 4000000
LN_EPS = 1e-5
F32 = jnp.float32
BF16 = jnp.bfloat16
MESH = pl.DeviceIdType.MESH
VMEM_LIMIT = 67043328

WBLK = 256
RING = 8
RBLK = 256
VBLK = 128
CHUNK = 128
KEYS = 512
VIA = 3
VIA_EXTRA = 16
VIA_AFTER = 6
VIA_PIECES = 9


def layer_kernel(x_hbm, gain_ref, pos_ref, freq_ref, wq_hbm, wk_hbm, wv_hbm, wo_hbm, wg_hbm, wu_hbm, wd_hbm,
                 out_hbm, k_hbm, v_hbm,
                 x_buf, h_buf, ring, act, q_buf, k_all, vt_all, v_own, wo, wd, recv, mlp, qs, o_buf, s_ref, blk_ref, top_ref, sum_ref, acc_ref,
                 x_sem, ring_sem, wo_sem, wd_sem, kv_sem, out_sem,
                 cross_send, cross_recv, up_send, up_recv, relay_send, relay_recv, part_send, part_recv, via, via_send, via_recv, cos_ref, sin_ref, swap):
    me = lax.axis_index("cp")
    tp = lax.axis_index("tp")
    odd = me % 2
    partner = me + 1 - 2 * odd
    across = (me + 2) % 4
    rows, width = x_buf.shape
    kv_heads = k_all.shape[0]
    n_rblk = rows // RBLK
    n_vblk = rows // VBLK
    n_piece = (n_vblk, kv_heads)
    n_chunk = rows // CHUNK
    n_ff = act.shape[1] // WBLK
    part = h_buf

    def x_copy(b):
        r = pl.ds(pl.multiple_of(b * VBLK, VBLK), VBLK)
        return pltpu.make_async_copy(x_hbm.at[r, :], x_buf.at[r, :], x_sem.at[b])

    def w_copy(w_hbm, blk, slot):
        c = pl.ds(pl.multiple_of(blk * WBLK, WBLK), WBLK)
        return pltpu.make_async_copy(w_hbm.at[:, c], ring.at[slot], ring_sem.at[slot])

    wo_copy = pltpu.make_async_copy(wo_hbm, wo, wo_sem)
    wd_copy = pltpu.make_async_copy(wd_hbm, wd, wd_sem)

    x_copy(0).start()
    w_copy(wv_hbm, 0, 0).start()
    w_copy(wv_hbm, 1, 1).start()
    for b in range(1, n_vblk):
        x_copy(b).start()
    for j in range(4):
        w_copy(wq_hbm, j, 4 + j).start()
    w_copy(wk_hbm, 0, 2).start()
    w_copy(wk_hbm, 1, 3).start()
    wo_copy.start()
    wd_copy.start()

    barrier = pltpu.get_barrier_semaphore()
    pl.semaphore_signal(barrier, inc=1, device_id={"tp": 1 - tp}, device_id_type=MESH)
    pl.semaphore_signal(barrier, inc=1, device_id={"cp": partner}, device_id_type=MESH)
    pl.semaphore_signal(barrier, inc=1, device_id={"cp": across}, device_id_type=MESH)

    def region(owner, kind, b):
        if kind:
            return k_all.at[b, pl.ds(pl.multiple_of(owner * rows, RBLK), rows), :]
        return vt_all.at[owner * n_vblk + b]

    def kv_copy(owner, kind, b, sends, recvs, target):
        ref = region(owner, kind, b)
        i = kind * n_vblk + b
        return pltpu.make_async_remote_copy(ref, ref, sends.at[i], recvs.at[i], device_id={"cp": target}, device_id_type=MESH)

    def cross(owner, kind, b):
        return kv_copy(owner, kind, b, cross_send, cross_recv, (owner + 2) % 4)

    def up(owner, kind, b):
        return kv_copy(owner, kind, b, up_send, up_recv, (owner + 1) % 4)

    def relay(owner, kind, b):
        return kv_copy(owner, kind, b, relay_send, relay_recv, 3 - owner)

    def send_piece(kind, b):
        @pl.when(me < 2)
        def _():
            cross(me, kind, b).start()

        @pl.when(odd == 0)
        def _():
            up(me, kind, b).start()

    def relay_piece(kind, b):
        owner = me - 2
        cross(owner, kind, b).wait_recv()
        kv_copy(owner, kind, b, relay_send, relay_recv, partner).start()

    def part_copy(c, n=CHUNK):
        r = pl.ds(pl.multiple_of(c * CHUNK, CHUNK), n)
        return pltpu.make_async_remote_copy(part.at[r, :], recv.at[r, :], part_send.at[c], part_recv.at[c],
                                            device_id={"tp": 1 - tp}, device_id_type=MESH)

    def for_part(c, act_on):
        upper = me >= 2
        short = upper & (c == VIA - 1)

        @pl.when(short)
        def _():
            act_on(part_copy(VIA - 1, CHUNK - VIA_EXTRA))

        @pl.when(jnp.logical_not(short | (upper & (c == VIA))))
        def _():
            act_on(part_copy(c))

    def via_copy(leg, i):
        n = VIA_EXTRA
        rows_i = slice(i * n, (i + 1) * n)
        at = slice(VIA * CHUNK + (i - 1) * n, VIA * CHUNK + i * n)
        src = (part.at[at, :], via.at[0, rows_i, :], via.at[1, rows_i, :])[leg]
        dst = (via.at[0, rows_i, :], via.at[1, rows_i, :], recv.at[at, :])[leg]
        target = {"tp": 1 - tp} if leg == 1 else {"cp": across}
        return pltpu.make_async_remote_copy(src, dst, via_send.at[leg * VIA_PIECES + i], via_recv.at[leg * VIA_PIECES + i],
                                            device_id=target, device_id_type=MESH)

    gain = jnp.concatenate([gain_ref[i:i + 1, :] for i in range(width // HEAD_DIM)], axis=1).astype(F32)

    def norm(b):
        r = pl.ds(pl.multiple_of(b * VBLK, VBLK), VBLK)
        x = x_buf[r, :].astype(F32)
        mean = jnp.mean(x, axis=-1, keepdims=True)
        cent = x - mean
        var = jnp.mean(cent * cent, axis=-1, keepdims=True)
        h_buf[r, :] = (cent * lax.rsqrt(var + LN_EPS) * gain).astype(BF16)

    def project_v(b):
        r = pl.ds(pl.multiple_of(b * VBLK, VBLK), VBLK)
        h = h_buf[r, :]
        for j in range(2):
            v = jnp.dot(h, ring[j], preferred_element_type=F32).astype(BF16)
            v_own[b % 2, :, j * WBLK:(j + 1) * WBLK] = v
            vt_all[me * n_vblk + b, j * WBLK:(j + 1) * WBLK, :] = v.T

    def v_copy(b):
        r = pl.ds(pl.multiple_of(b * VBLK, VBLK), VBLK)
        return pltpu.make_async_copy(v_own.at[b % 2], v_hbm.at[r, :], kv_sem.at[b % 2])

    x_copy(0).wait()
    norm(0)
    w_copy(wv_hbm, 0, 0).wait()
    w_copy(wv_hbm, 1, 1).wait()
    pl.semaphore_wait(barrier, 3)

    @pl.loop(0, n_vblk - 1)
    def _(b):
        x_copy(b + 1).wait()

        @pl.when(b >= 2)
        def _():
            v_copy(b - 2).wait()

        project_v(b)
        norm(b + 1)
        send_piece(0, b)
        v_copy(b).start()

    v_copy(n_vblk - 3).wait()
    project_v(n_vblk - 1)
    send_piece(0, n_vblk - 1)
    v_copy(n_vblk - 1).start()

    def ff_copies(s):
        slot = 2 * (s % 4)
        return w_copy(wg_hbm, s % n_ff, slot), w_copy(wu_hbm, s % n_ff, slot + 1)

    def ff_start(s):
        for copy in ff_copies(s):
            copy.start()

    ff_start(0)
    sign = jnp.where(lax.broadcasted_iota(jnp.int32, (1, HEAD_DIM), 1) % 2 == 0, -1.0, 1.0).astype(F32)

    @pl.loop(0, 4)
    def _(j):
        w_copy(wq_hbm, j, 4 + j).wait()
        for b in range(n_rblk):
            r = slice(b * RBLK, (b + 1) * RBLK)
            cols = pl.ds(pl.multiple_of(j * WBLK, WBLK), WBLK)
            q_buf[r, cols] = jnp.dot(h_buf[r, :], ring[4 + j], preferred_element_type=F32).astype(BF16)
        for i in range(2):
            row = 2 * j + i
            pos = jnp.broadcast_to(pos_ref[pl.ds(row, 1), :].astype(F32), (HEAD_DIM, HEAD_DIM)).T
            angle = pos * freq_ref[...]
            at = pl.ds(pl.multiple_of(row * HEAD_DIM, HEAD_DIM), HEAD_DIM)
            cos_ref[at, :] = jnp.cos(angle)
            sin_ref[at, :] = jnp.sin(angle) * sign

    ff_start(2)
    ff_start(3)

    lane = lax.broadcasted_iota(jnp.int32, (WBLK, WBLK), 0)
    other = lax.broadcasted_iota(jnp.int32, (WBLK, WBLK), 1)
    swap[...] = jnp.where(lane == other + 1 - 2 * (other % 2), 1.0, 0.0).astype(BF16)

    def rotate(proj, swapped, r):
        cos = cos_ref[r, :]
        sin = sin_ref[r, :]
        heads = [slice(i * HEAD_DIM, (i + 1) * HEAD_DIM) for i in range(WBLK // HEAD_DIM)]
        return [(proj[:, c].astype(F32) * cos + swapped[:, c] * sin).astype(BF16) for c in heads]

    @pl.loop(0, 2)
    def _(j):
        w_copy(wk_hbm, j, 2 + j).wait()
        proj = [None] * n_rblk

        def project(b):
            proj[b] = jnp.dot(h_buf[b * RBLK:(b + 1) * RBLK, :], ring[2 + j], preferred_element_type=F32).astype(BF16)

        project(0)
        for b in range(n_rblk):
            if b + 1 < n_rblk:
                project(b + 1)
            swapped = jnp.dot(proj[b], swap[...], preferred_element_type=F32)
            at = pl.ds(pl.multiple_of(me * rows + b * RBLK, RBLK), RBLK)
            for i, k in enumerate(rotate(proj[b], swapped, slice(b * RBLK, (b + 1) * RBLK))):
                k_all[2 * j + i, at, :] = k
        send_piece(1, 2 * j)
        send_piece(1, 2 * j + 1)

    ff_start(1)
    def k_copy(g):
        return pltpu.make_async_copy(k_all.at[g, pl.ds(pl.multiple_of(me * rows, RBLK), rows), :],
                                     k_hbm.at[:, g * HEAD_DIM:(g + 1) * HEAD_DIM], kv_sem.at[2 + g])

    for g in range(kv_heads):
        k_copy(g).start()

    relay_steps = ((12, 0, 0), (12, 0, 1), (12, 0, 2), (12, 0, 3), (14, 0, 4), (16, 0, 5), (19, 0, 6), (21, 0, 7),
                   (26, 1, 0), (30, 1, 1), (34, 1, 2))
    n_steps = 3 * n_ff

    def feed(first_step, first_block, n_blocks):
        @pl.loop(first_step, first_step + n_ff)
        def _(s):
            for copy in ff_copies(s):
                copy.wait()
            slot = 2 * (s % 4)
            for b in range(n_blocks):
                r = pl.ds(pl.multiple_of((first_block + b) * RBLK, RBLK), RBLK)
                h = h_buf[r, :]
                gate = jnp.dot(h, ring[slot], preferred_element_type=F32).astype(BF16).astype(F32)
                up_ = jnp.dot(h, ring[slot + 1], preferred_element_type=F32).astype(BF16).astype(F32)
                act[r, pl.ds(pl.multiple_of((s % n_ff) * WBLK, WBLK), WBLK)] = (jax.nn.silu(gate) * up_).astype(BF16)

            @pl.when(s + 4 < n_steps)
            def _():
                ff_start(s + 4)

            for step, kind, b in relay_steps:
                @pl.when((me >= 2) & (s == step))
                def _():
                    relay_piece(kind, b)

    def down(c):
        r = pl.ds(pl.multiple_of(c * CHUNK, CHUNK), CHUNK)
        a = act[r, :]
        for j in range(4):
            cols = slice(j * (width // 4), (j + 1) * (width // 4))
            mlp[:, cols] = jnp.dot(a, wd[:, cols], preferred_element_type=F32)

    scale = HEAD_DIM ** -0.5 * math.log2(math.e)

    low = jnp.where(me < 2, 0, 2 * (rows // KEYS))

    def head(g):
        return slice(g * HEAD_DIM, (g + 1) * HEAD_DIM)

    def key_rows(j):
        return pl.ds(pl.multiple_of(j * KEYS, KEYS), KEYS)

    def score(j, g):
        s = lax.dot_general(k_all[g, key_rows(j), :], qs[g], (((1,), (1,)), ((), ())), preferred_element_type=F32)
        s_ref[g] = s
        blk_ref[g] = jnp.max(s, axis=0, keepdims=True)

    def weigh(g, s, block_top):
        old = top_ref[g]
        new = jnp.maximum(old, block_top)
        factor = jnp.exp2((old - new) * scale)
        weight = jnp.exp2((s - new) * scale)
        top_ref[g] = new
        sum_ref[g] = sum_ref[g] * factor + jnp.sum(weight, axis=0, keepdims=True)
        return factor, weight.astype(BF16)

    def collect(j, g, factor, weight):
        vt = jnp.concatenate([vt_all[j * (KEYS // VBLK) + i, head(g), :] for i in range(KEYS // VBLK)], axis=1)
        acc_ref[g] = acc_ref[g] * factor + jnp.dot(vt, weight, preferred_element_type=F32)

    def chunk(c, stop):
        r = pl.ds(pl.multiple_of(c * CHUNK, CHUNK), CHUNK)
        swapped = [jnp.dot(q_buf[r, g * WBLK:(g + 1) * WBLK], swap[...], preferred_element_type=F32) for g in range(kv_heads)]
        for g in range(kv_heads):
            for i, q in enumerate(rotate(q_buf[r, g * WBLK:(g + 1) * WBLK], swapped[g], r)):
                qs[g, i * CHUNK:(i + 1) * CHUNK, :] = q
        top_ref[...] = jnp.full_like(top_ref, -jnp.inf)
        sum_ref[...] = jnp.zeros_like(sum_ref)
        acc_ref[...] = jnp.zeros_like(acc_ref)
        full = me * (rows // KEYS) + c // (KEYS // CHUNK)
        for g in range(kv_heads):
            score(low, g)

        def step(j):
            for g in range(kv_heads):
                factor, weight = weigh(g, s_ref[g], blk_ref[g])
                score(j + 1, g)
                collect(j, g, factor, weight)

        @pl.loop(low, full)
        def _(j):
            step(j)

        first = (c % (KEYS // CHUNK)) * CHUNK
        key_id = lax.broadcasted_iota(jnp.int32, (KEYS, 2 * CHUNK), 0)
        query_id = lax.broadcasted_iota(jnp.int32, (KEYS, 2 * CHUNK), 1) % CHUNK
        for g in range(kv_heads):
            s = jnp.where(key_id <= query_id + first, s_ref[g], -jnp.inf)
            factor, weight = weigh(g, s, jnp.max(s, axis=0, keepdims=True))
            collect(full, g, factor, weight)

        @pl.when(me >= 2)
        def _():
            @pl.when(c == 0)
            def _():
                relay_piece(1, 3)
                for kind in range(2):
                    for b in range(n_piece[kind]):
                        kv_copy(3 - me, kind, b, relay_send, relay_recv, partner).wait_recv()

            for g in range(kv_heads):
                score(0, g)

            @pl.loop(0, low)
            def _(j):
                step(j)

        for g in range(kv_heads):
            o = (acc_ref[g] / sum_ref[g]).T.astype(BF16)
            for i in range(2):
                col = (2 * g + i) * HEAD_DIM
                o_buf[:, col:col + HEAD_DIM] = o[i * CHUNK:(i + 1) * CHUNK, :]
        o = o_buf[...]
        for j in range(4):
            cols = slice(j * (width // 4), (j + 1) * (width // 4))
            part[r, cols] = (jnp.dot(o, wo[:, cols], preferred_element_type=F32) + mlp[:, cols]).astype(BF16)

        for_part(c, lambda copy: copy.start())

        @pl.when((me >= 2) & (c == VIA - 1))
        def _():
            via_copy(0, 0).start()

        @pl.when((me >= 2) & (c == VIA))
        def _():
            for i in range(1, VIA_PIECES):
                via_copy(0, i).start()

        @pl.when((me < 2) & (c == VIA_AFTER))
        def _():
            for i in range(VIA_PIECES):
                via_copy(0, i).wait_recv()
                via_copy(1, i).start()

        @pl.when(c + 1 < stop)
        def _():
            down(c + 1)

    per_block = RBLK // CHUNK
    early = jnp.where(me < 2, 2, 0)

    def await_weights():
        wo_copy.wait()
        wd_copy.wait()

        @pl.when(odd == 1)
        def _():
            for kind in range(2):
                for b in range(n_piece[kind]):
                    up(me - 1, kind, b).wait_recv()

    @pl.loop(0, early)
    def _(block):
        feed(block * n_ff, block, 1)

        @pl.when(block == 0)
        def _():
            await_weights()

        first = block * per_block
        down(first)

        @pl.loop(first, first + per_block)
        def _(c):
            chunk(c, first + per_block)

    @pl.when(me >= 2)
    def _():
        feed(n_ff, 0, 2)
        await_weights()

    feed(2 * n_ff, 2, 2)
    down(early * per_block)

    @pl.loop(early * per_block, n_chunk)
    def _(c):
        chunk(c, n_chunk)

    def out_copy(c):
        r = pl.ds(pl.multiple_of(c * CHUNK, CHUNK), CHUNK)
        return pltpu.make_async_copy(x_buf.at[r, :], out_hbm.at[r, :], out_sem.at[c])

    def finish(c):
        for i in range(4):
            n = CHUNK // 4
            r = pl.ds(pl.multiple_of(c * CHUNK + i * n, n), n)
            x_buf[r, :] = (x_buf[r, :].astype(F32) + (part[r, :].astype(F32) + recv[r, :].astype(F32))).astype(BF16)
            pltpu.make_async_copy(x_buf.at[r, :], out_hbm.at[r, :], out_sem.at[c]).start()

    @pl.loop(0, n_chunk)
    def _(c):
        @pl.when((me < 2) & (c == VIA_AFTER + 1))
        def _():
            for i in range(VIA_PIECES):
                via_copy(1, i).wait_recv()
                via_copy(2, i).start()

        @pl.when((me >= 2) & (c == n_chunk - 1))
        def _():
            for i in range(VIA_PIECES):
                via_copy(2, i).wait_recv()
            finish(VIA - 1)
            finish(VIA)

        for_part(c, lambda copy: copy.wait_recv())

        @pl.when((me < 2) | ((c != VIA) & (c != VIA - 1)))
        def _():
            finish(c)

    @pl.loop(0, n_chunk)
    def _(c):
        out_copy(c).wait()

        for_part(c, lambda copy: copy.wait_send())

    for i in range(VIA_PIECES):
        @pl.when(me >= 2)
        def _():
            via_copy(0, i).wait_send()

        @pl.when(me < 2)
        def _():
            via_copy(1, i).wait_send()
            via_copy(2, i).wait_send()

    v_copy(n_vblk - 2).wait()
    v_copy(n_vblk - 1).wait()
    for g in range(kv_heads):
        k_copy(g).wait()
    for kind in range(2):
        for b in range(n_piece[kind]):
            @pl.when(me < 2)
            def _():
                cross(me, kind, b).wait_send()

            @pl.when(odd == 0)
            def _():
                up(me, kind, b).wait_send()

            @pl.when(me >= 2)
            def _():
                kv_copy(me - 2, kind, b, relay_send, relay_recv, partner).wait_send()


def place_kernel(m_ref, k_ref, v_ref, out_ref, kc_ref, vc_ref):
    out_ref[...] = m_ref[...]
    kc_ref[...] = k_ref[...].reshape(kc_ref.shape)
    vc_ref[...] = v_ref[...].reshape(vc_ref.shape)


def place(out, k, v, kv_heads):
    rows, width = out.shape
    blk = 512
    kv_spec = pl.BlockSpec((blk, k.shape[1]), lambda i: (i, 0))
    cache_spec = pl.BlockSpec((blk, kv_heads, HEAD_DIM), lambda i: (i, 0, 0))
    cache = jax.ShapeDtypeStruct((rows, kv_heads, HEAD_DIM), BF16)
    return pl.pallas_call(
        place_kernel,
        grid=(rows // blk,),
        in_specs=[pl.BlockSpec((blk, width), lambda i: (i, 0)), kv_spec, kv_spec],
        out_specs=[pl.BlockSpec((blk, width), lambda i: (i, 0)), cache_spec, cache_spec],
        out_shape=[jax.ShapeDtypeStruct((rows, width), BF16), cache, cache],
        compiler_params=pltpu.CompilerParams(dimension_semantics=("arbitrary",)),
        name="place",
    )(out, k, v)


def solution(mesh):
    n_cp = mesh.shape['cp']

    def local_layer(hidden, positions, ln_gain, w_q, w_k, w_v, w_o, w_gate, w_up, w_down):
        rows, width = hidden.shape
        q_cols = w_q.shape[1]
        kv_cols = w_k.shape[1]
        ff = w_gate.shape[1]
        kv_heads = kv_cols // HEAD_DIM
        keys = n_cp * rows
        n_chunk = rows // CHUNK
        pieces = rows // VBLK + kv_heads
        lane = np.arange(HEAD_DIM)
        inv_freq = (1.0 / ROPE_BASE ** ((lane - lane % 2) / HEAD_DIM)).astype(np.float32)
        hbm = pl.BlockSpec(memory_space=pl.ANY)
        vmem = pl.BlockSpec(memory_space=pltpu.VMEM)
        dma = pltpu.SemaphoreType.DMA
        out, k, v = pl.pallas_call(
            layer_kernel,
            in_specs=[hbm, vmem, vmem, vmem] + [hbm] * 7,
            out_specs=[hbm] * 3,
            out_shape=[
                jax.ShapeDtypeStruct((rows, width), BF16),
                jax.ShapeDtypeStruct((rows, kv_cols), BF16),
                jax.ShapeDtypeStruct((rows, kv_cols), BF16),
            ],
            scratch_shapes=[
                pltpu.VMEM((rows, width), BF16),
                pltpu.VMEM((rows, width), BF16),
                pltpu.VMEM((RING, width, WBLK), BF16),
                pltpu.VMEM((rows, ff), BF16),
                pltpu.VMEM((rows, q_cols), BF16),
                pltpu.VMEM((kv_heads, keys, HEAD_DIM), BF16),
                pltpu.VMEM((keys // VBLK, kv_cols, VBLK), BF16),
                pltpu.VMEM((2, VBLK, kv_cols), BF16),
                pltpu.VMEM((q_cols, width), BF16),
                pltpu.VMEM((ff, width), BF16),
                pltpu.VMEM((rows, width), BF16),
                pltpu.VMEM((CHUNK, width), F32),
                pltpu.VMEM((kv_heads, 2 * CHUNK, HEAD_DIM), BF16),
                pltpu.VMEM((CHUNK, q_cols), BF16),
                pltpu.VMEM((kv_heads, KEYS, 2 * CHUNK), F32),
                pltpu.VMEM((kv_heads, 1, 2 * CHUNK), F32),
                pltpu.VMEM((kv_heads, 1, 2 * CHUNK), F32),
                pltpu.VMEM((kv_heads, 1, 2 * CHUNK), F32),
                pltpu.VMEM((kv_heads, HEAD_DIM, 2 * CHUNK), F32),
                dma((rows // VBLK,)), dma((RING,)), dma, dma, dma((2 + kv_heads,)), dma((n_chunk,)),
                dma((pieces,)), dma((pieces,)), dma((pieces,)), dma((pieces,)), dma((pieces,)), dma((pieces,)),
                dma((n_chunk,)), dma((n_chunk,)),
                pltpu.VMEM((2, VIA_EXTRA * VIA_PIECES, width), BF16), dma((3 * VIA_PIECES,)), dma((3 * VIA_PIECES,)),
                pltpu.VMEM((rows, HEAD_DIM), F32), pltpu.VMEM((rows, HEAD_DIM), F32), pltpu.VMEM((WBLK, WBLK), BF16),
            ],
            compiler_params=pltpu.CompilerParams(collective_id=0, has_side_effects=True, vmem_limit_bytes=VMEM_LIMIT),
            name="layer",
        )(hidden, ln_gain.reshape(width // HEAD_DIM, HEAD_DIM), positions.reshape(rows // HEAD_DIM, HEAD_DIM), jnp.asarray(inv_freq[None, :]), w_q, w_k, w_v, w_o, w_gate, w_up, w_down)
        return place(out, k, v, kv_heads)

    row_spec = P(('dp', 'cp'), None)
    col_spec = P(None, 'tp')
    cache_spec = P(('dp', 'cp'), 'tp', None)
    in_specs = (row_spec, P(('dp', 'cp')), P(None), col_spec, col_spec, col_spec, P('tp', None), col_spec, col_spec, P('tp', None))
    return jax.shard_map(local_layer, mesh=mesh, in_specs=in_specs, out_specs=(row_spec, cache_spec, cache_spec), check_vma=False)
```
